256 devices in a mesh: dir: 32 (over z, x), coil: 8 (over y, core).
Axes of the slice: x: 4, y: 4, z: 8, core: 2. Of those that a mesh axis runs over, the one named last changes fastest.
Arguments:
- kspace: bfloat16 [64, 8, 32, 128, 512], P(None, None, 'coil', 'dir'), may hold values from -6 to 6
- accept: int32 [64, 8], replicated, may hold values from 0 to 1, as said below
- trajectory: int32 [64, 8, 128], P('dir'), may hold values from 0 to 255
- phase_coef: float32 [64, 8, 16, 16], P('dir'), may hold values from -2 to 2
- sens: bfloat16 [32, 256, 512], P('coil'), may hold values from -1.1953125 to 1.1953125
Outputs:
- image: float32 [64, 256, 512], P('dir', 'coil')
The draws below stay inside these ranges and needn't reach their ends.
Inputs may be any that keep to these rules, and one draw needn't show every extreme that they name: `accept`: each direction accepts 1 to 6 of its 8 shots, and some direction accepts exactly 6.
All inputs are finite; a program needn't handle non-finite values.
Results may differ from the reference program's by a relative error of at most 0.0043.
Values may be sent and summed in bfloat16 or wider, within the bound.
A program may use at most 128 MiB of HBM per device.

```python
import math
import jax
import jax.numpy as jnp
from jax import lax

IMG = 256
ROWS = 128
COILS = 32
SHOTS = 8
ACCEPTED = 6
PB = 16
DIRS = 64


def draw_accept(key, part):
    base = jax.random.fold_in(key, 11)
    first, second, third = jax.random.split(base, 3)
    counts = jax.random.randint(first, (DIRS,), 1, ACCEPTED + 1)
    chosen = jax.random.randint(second, (), 0, DIRS)
    counts = jnp.where(jnp.arange(DIRS) == chosen, ACCEPTED, counts)
    scores = jax.random.randint(third, (DIRS, SHOTS), 0, 1 << 20) * SHOTS + jnp.arange(SHOTS)[None, :]
    ranking = jnp.argsort(jnp.argsort(scores, axis=1), axis=1)
    return (ranking < counts[:, None]).astype(jnp.int32)


def place_ends(entries, key, smallest, top_value):
    place = [jax.random.randint(jax.random.fold_in(key, axis), (), 0, length) for axis, length in enumerate(entries.shape)]
    widest = entries.shape.index(max(entries.shape))
    next_to = place[:widest] + [(place[widest] + 1) % entries.shape[widest]] + place[widest + 1:]
    return entries.at[tuple(place)].set(smallest).at[tuple(next_to)].set(top_value)


def shard_levels(key, dims, shards, low, top_value):
    gain = 1.0
    for axis_at, shards_of in shards:
        heights = jax.random.uniform(jax.random.fold_in(jax.random.fold_in(key, 6), axis_at), (shards_of,), jnp.float32, low / len(shards), top_value / len(shards))
        gain = gain * jnp.repeat(jnp.exp(heights), dims[axis_at] // shards_of).reshape((-1,) + (1,) * (len(dims) - 1 - axis_at))
    return gain


def centred(stream_key, dims, deviation, most, cuts=(), kind=jnp.bfloat16):
    values = deviation * jax.random.normal(stream_key, dims, jnp.float32)
    if cuts:
        values = values * shard_levels(stream_key, dims, cuts, -0.22, 0.18)
    return jnp.clip(values, -most, most).astype(kind)


def setup_inputs(seed: int = 0) -> dict:
    key_list = jax.random.split(jax.random.key(seed), 6)
    kspace = centred(key_list[0], (DIRS, SHOTS, COILS, ROWS, 2 * IMG), 1.0, 6.0, ((2, 8), (3, 32)))
    accept = draw_accept(jax.random.fold_in(key_list[5], 71), 0)
    trajectory = place_ends(jax.random.randint(key_list[2], (DIRS, SHOTS, ROWS), 0, IMG), jax.random.fold_in(key_list[2], 1), 0, IMG - 1).astype(jnp.int32)
    phase_coef = centred(key_list[3], (DIRS, SHOTS, PB, PB), 0.3, 2.0, ((0, 32),), jnp.float32)
    sens = centred(key_list[4], (COILS, IMG, 2 * IMG), 0.2, 1.1953125, ((0, 8),))
    return dict(kspace=kspace, accept=accept, trajectory=trajectory, phase_coef=phase_coef, sens=sens)


def readout_table(size):
    points = jnp.arange(size, dtype=jnp.int32)
    product = points[:, None] * points[None, :] % size
    angles = product.astype(jnp.float32) * (2.0 * math.pi / size)
    cosine = jnp.cos(angles)
    sine = jnp.sin(angles)
    upper = jnp.concatenate([cosine, sine], 1)
    lower = jnp.concatenate([-sine, cosine], 1)
    return jnp.concatenate([upper, lower], 0).astype(jnp.bfloat16)

def line_tables(ky_lines, size):
    points = jnp.arange(size, dtype=jnp.int32)
    product = ky_lines[:, None].astype(jnp.int32) * points[None, :] % size
    angles = product.astype(jnp.float32) * (2.0 * math.pi / size)
    return (jnp.cos(angles).astype(jnp.bfloat16), jnp.sin(angles).astype(jnp.bfloat16))

def cosine_basis(size, terms):
    points = jnp.arange(size, dtype=jnp.int32).astype(jnp.float32)
    orders = jnp.arange(terms, dtype=jnp.int32).astype(jnp.float32)
    return jnp.cos(math.pi * orders[None, :] * (points[:, None] + 0.5) / size)

def shot_image(shot_data, ky_lines, readout_tab, sens):
    coils, row_count, width = shot_data.shape
    halfwidth = width // 2
    spectra = jnp.dot(shot_data.reshape(coils * row_count, width), readout_tab, preferred_element_type=jnp.float32)
    spectra = (spectra * (1.0 / math.sqrt(halfwidth))).astype(jnp.bfloat16).reshape(coils, row_count, width)
    swapped = jnp.concatenate([-spectra[..., halfwidth:], spectra[..., :halfwidth]], -1)
    cos_tab, sin_tab = line_tables(ky_lines, halfwidth)
    coil_images = jnp.einsum('ry,crx->cyx', cos_tab.astype(jnp.float32), spectra.astype(jnp.float32))
    coil_images = coil_images + jnp.einsum('ry,crx->cyx', sin_tab.astype(jnp.float32), swapped.astype(jnp.float32))
    coil_images = coil_images * (1.0 / math.sqrt(row_count))
    sens_re = sens[..., :halfwidth].astype(jnp.float32)
    sens_im = sens[..., halfwidth:].astype(jnp.float32)
    image_re = coil_images[..., :halfwidth]
    image_im = coil_images[..., halfwidth:]
    unit_re = lax.optimization_barrier(jnp.sum(sens_re * image_re + sens_im * image_im, 0))
    unit_im = lax.optimization_barrier(jnp.sum(sens_re * image_im - sens_im * image_re, 0))
    return jnp.concatenate([unit_re, unit_im], -1)

def phase_apply(images, coefs, weights, basis_rows, basis_cols):
    halfwidth = images.shape[2] // 2
    partial_map = jnp.einsum('yk,skl->syl', basis_rows, coefs, precision=lax.Precision.HIGHEST)
    angles = jnp.einsum('syl,xl->syx', partial_map, basis_cols, precision=lax.Precision.HIGHEST)
    cosine = jnp.cos(angles)
    sine = jnp.sin(angles)
    unit_re = images[..., :halfwidth]
    unit_im = images[..., halfwidth:]
    scaled = weights.astype(jnp.float32)[:, None, None]
    out_re = lax.optimization_barrier(jnp.sum(scaled * (cosine * unit_re + sine * unit_im), 0)) / SHOTS
    out_im = lax.optimization_barrier(jnp.sum(scaled * (cosine * unit_im - sine * unit_re), 0)) / SHOTS
    return jnp.concatenate([out_re, out_im], -1)

def reference(kspace, accept, trajectory, phase_coef, sens):
    readout_tab = readout_table(IMG)
    basis_full = cosine_basis(IMG, PB)

    def one_direction(packed):
        blocks, flags, ky_rows, coefs = packed
        images = lax.map(lambda pair: shot_image(pair[0], pair[1], readout_tab, sens), (blocks, ky_rows))
        return phase_apply(images, coefs, flags, basis_full, basis_full)
    return lax.map(one_direction, (kspace, accept, trajectory, phase_coef))
```

```python
import functools
import math

import jax
import jax.numpy as jnp
import numpy as np
from jax import lax
from jax.experimental import pallas as pl
from jax.experimental.pallas import tpu as pltpu
from jax.sharding import Mesh, PartitionSpec as P

IMG = 256
SHOTS = 8
PB = 16
DIRS = 64
HALF = IMG // 2
MESH = pl.DeviceIdType.MESH
AXES = ("zh", "zl", "x", "y", "core")
BF = jnp.bfloat16
F32 = jnp.float32

LEVELS = (32, 36, 40, 48)
STEP = {32: 16, 36: 18, 40: 20, 48: 16}


def readout_const():
    k = np.arange(IMG)
    ang = (np.outer(k, k) % IMG).astype(np.float64) * (2.0 * np.pi / IMG)
    c, s = np.cos(ang).astype(np.float32), np.sin(ang).astype(np.float32)
    tab = np.concatenate([np.concatenate([c, s], 1), np.concatenate([-s, c], 1)], 0)
    order = np.concatenate([np.arange(HALF), IMG + np.arange(HALF), HALF + np.arange(HALF), IMG + HALF + np.arange(HALF)])
    return jnp.asarray(tab[:, order]).astype(BF)


def line_const():
    k = np.arange(IMG)
    ang = (np.outer(k, k) % IMG).astype(np.float64) * (2.0 * np.pi / IMG)
    return jnp.asarray(np.concatenate([np.cos(ang), np.sin(ang)], 1).astype(np.float32)).astype(BF)


def basis_const():
    points = np.arange(IMG, dtype=np.float64)
    orders = np.arange(PB, dtype=np.float64)
    return np.cos(np.pi * orders[None, :] * (points[:, None] + 0.5) / IMG)


def split3(a):
    one = np.asarray(a, np.float32).astype(BF)
    rest = np.asarray(a, np.float64) - one.astype(np.float64)
    two = rest.astype(np.float32).astype(BF)
    rest = rest - two.astype(np.float64)
    return one, two, rest.astype(np.float32).astype(BF)


def poly_consts():
    u = np.cos(np.linspace(0, np.pi, 4001)) * 0.125 + 0.125
    t = np.sqrt(np.maximum(u, 0))
    fs = np.where(t > 1e-9, np.sin(2 * np.pi * t) / np.where(t > 1e-9, t, 1), 2 * np.pi)
    return [float(v) for v in np.polyfit(u, fs, 5)], [float(v) for v in np.polyfit(u, np.cos(2 * np.pi * t), 6)]


SIN_C, COS_C = poly_consts()


def sincos_turns(turns):
    t = turns - jnp.round(turns)
    u = t * t
    s = jnp.full_like(u, SIN_C[0])
    for v in SIN_C[1:]:
        s = s * u + v
    c = jnp.full_like(u, COS_C[0])
    for v in COS_C[1:]:
        c = c * u + v
    return s * t, c


def readout_kernel(count, idx_ref, tab_ref, *refs):
    out_ref = refs[count]
    rows = jnp.concatenate([refs[i][0] for i in range(count)], 0)
    spec = jnp.dot(rows, tab_ref[...], preferred_element_type=F32) * (1.0 / math.sqrt(IMG))
    spec = spec.astype(BF).reshape(count, 16, 2 * IMG)
    out_ref[0, 0, 0] = spec[:, :, :IMG]
    out_ref[0, 1, 0] = spec[:, :, IMG:]


def readout(slots, kspace, index, tab):
    count = STEP[slots]

    def pick(i, q, p, b, idx):
        return (idx[((q * 2 + p) * (slots // count) + b) * count + i], 0, 0)

    return pl.pallas_call(
        functools.partial(readout_kernel, count),
        grid_spec=pltpu.PrefetchScalarGridSpec(
            num_scalar_prefetch=1,
            grid=(4, 2, slots // count),
            in_specs=[pl.BlockSpec((2 * IMG, 2 * IMG), lambda q, p, b, idx: (0, 0))]
            + [pl.BlockSpec((1, 16, 2 * IMG), functools.partial(pick, i)) for i in range(count)],
            out_specs=pl.BlockSpec((1, 2, 1, count, 16, IMG), lambda q, p, b, idx: (q, 0, p, b, 0, 0)),
        ),
        out_shape=jax.ShapeDtypeStruct((4, 2, 2, slots, 16, IMG), BF),
        cost_estimate=pl.CostEstimate(flops=8 * slots * 16 * 512 * 512 * 2, bytes_accessed=8 * slots * 16 * 512 * 4, transcendentals=0),
        name="readout",
    )(index, tab, *([kspace] * count))


def partner(p, i, n):
    if p == 0:
        return i + 1 - 2 * lax.rem(i, 2)
    return lax.rem(i + 2 * lax.rem(i, 2) - 1 + n, n)


def exchange_kernel(slots, send_ref, sens_ref, recv_ref, both_ref, keep, keep_sens, send_sem, recv_sem, local_sem):
    zh, zl = lax.axis_index("zh"), lax.axis_index("zl")
    x, y, core = lax.axis_index("x"), lax.axis_index("y"), lax.axis_index("core")
    z = zh * 2 + zl
    src = lax.rem(x, 2) * 2 + zl

    def target(p, bits):
        bx, bz, bc = bits
        tx = partner(p, x, 4) if bx else x
        tz = partner(p, z, 8) if bz else z
        tc = 1 - core if bc else core
        return tz, tx, tc

    def device(p, bits):
        tz, tx, tc = target(p, bits)
        return (tz // 2, lax.rem(tz, 2), tx, y, tc)

    every = [(p, (bx, bz, bc)) for bx in (1, 0) for bz in (1, 0) for bc in (0, 1) for p in (0, 1) if bx + bz + bc]
    barrier = pltpu.get_barrier_semaphore()
    for p, bits in every:
        pl.semaphore_signal(barrier, inc=1, device_id=device(p, bits), device_id_type=MESH)
    pl.semaphore_wait(barrier, len(every))

    copies = []
    for n, (p, bits) in enumerate(every):
        tz, tx, tc = target(p, bits)
        copies.append(
            pltpu.make_async_remote_copy(
                src_ref=send_ref.at[lax.rem(tz, 2) * 2 + tc, lax.rem(tx, 2), p],
                dst_ref=recv_ref.at[p, src, core],
                send_sem=send_sem.at[n],
                recv_sem=recv_sem.at[n],
                device_id=device(p, bits),
                device_id_type=MESH,
            )
        )
    n = len(every)
    copies.append(
        pltpu.make_async_remote_copy(
            src_ref=sens_ref,
            dst_ref=both_ref.at[core],
            send_sem=send_sem.at[n],
            recv_sem=recv_sem.at[n],
            device_id=(zh, zl, x, y, 1 - core),
            device_id_type=MESH,
        )
    )
    for copy in copies:
        copy.start()
    loads = [
        pltpu.make_async_copy(send_ref.at[zl * 2 + core, lax.rem(x, 2), p], keep.at[p], local_sem.at[p])
        for p in (0, 1)
    ] + [pltpu.make_async_copy(sens_ref, keep_sens, local_sem.at[2])]
    stores = [
        pltpu.make_async_copy(keep.at[p], recv_ref.at[p, src, core], local_sem.at[3 + p]) for p in (0, 1)
    ] + [pltpu.make_async_copy(keep_sens, both_ref.at[core], local_sem.at[5])]
    for load in loads:
        load.start()
    for load, store in zip(loads, stores):
        load.wait()
        store.start()
    for store in stores:
        store.wait()
    for copy in copies:
        copy.wait()


def exchange(slots, ident, send, sens):
    return pl.pallas_call(
        functools.partial(exchange_kernel, slots),
        in_specs=[pl.BlockSpec(memory_space=pl.ANY)] * 2,
        out_specs=[pl.BlockSpec(memory_space=pl.ANY)] * 2,
        out_shape=[
            jax.ShapeDtypeStruct((2, 4, 2, slots, 16, IMG), BF),
            jax.ShapeDtypeStruct((2, 4, IMG, IMG), BF),
        ],
        scratch_shapes=[
            pltpu.VMEM((2, slots, 16, IMG), BF),
            pltpu.VMEM((4, IMG, IMG), BF),
            pltpu.SemaphoreType.DMA((15,)),
            pltpu.SemaphoreType.DMA((15,)),
            pltpu.SemaphoreType.DMA((6,)),
        ],
        compiler_params=pltpu.CompilerParams(collective_id=ident, has_side_effects=True),
        name="exchange",
    )(send, sens)


YB = 64


def image_kernel(slots, meta_ref, data_ref, sens_ref, traj_ref, coef_ref, line_ref, basy_ref, basx_ref, out_ref, acc, sens, weights):
    total = meta_ref[0]
    acc[...] = jnp.zeros_like(acc)
    scale = 1.0 / (math.sqrt(128.0) * SHOTS)
    for s in range(2):
        for c in range(4):
            sens[s, :, c * YB:(c + 1) * YB, :] = (sens_ref[s, c].astype(F32) * scale).reshape(4, YB, IMG)
    lane = lax.broadcasted_iota(jnp.int32, (IMG, HALF), 1)
    coil = lax.rem(lane // 4, 4)
    masks = [coil == c for c in range(4)]
    kline = lax.broadcasted_iota(jnp.int32, (2 * IMG, HALF), 0)

    def unit(j, carry):
        code = meta_ref[1 + j]
        p = lax.rem(j, 2)
        slot = j // 2
        direction = code // SHOTS
        pick = (kline == traj_ref[code * 2 + p]).astype(F32).astype(BF)
        table = jnp.dot(line_ref[...], pick, preferred_element_type=F32)
        for c in range(4):
            weights[:, c * YB:(c + 1) * YB, :] = jnp.where(masks[c], table, 0.0).astype(BF).reshape(4, YB, HALF)
        coefs = coef_ref[code]
        mixed = jnp.dot(coefs, basx_ref[...], preferred_element_type=F32, precision=lax.Precision.HIGHEST)
        one = mixed.astype(BF)
        rest = mixed - one.astype(F32)
        two = rest.astype(BF)
        three = (rest - two.astype(F32)).astype(BF)
        mixed6 = jnp.concatenate([one, two, one, two, three, one], 0)
        rhs = []
        for s in range(2):
            rows = jnp.concatenate([data_ref[p, w, s, slot] for w in range(4)], 0)
            swapped = jnp.concatenate([-rows[:, HALF:], rows[:, :HALF]], 1)
            rhs.append(jnp.concatenate([rows, swapped], 0))

        for b in range(IMG // YB):
            turns = jnp.dot(basy_ref[b * YB:(b + 1) * YB, :], mixed6, preferred_element_type=F32)
            sine, cosine = sincos_turns(turns)
            ure = jnp.zeros((YB, HALF), F32)
            uim = jnp.zeros((YB, HALF), F32)
            for s in range(2):
                image = jnp.dot(weights[b], rhs[s], preferred_element_type=F32)
                for c in range(4):
                    ire, iim = image[c * YB:(c + 1) * YB, :HALF], image[c * YB:(c + 1) * YB, HALF:]
                    sre = sens[s, b, c * YB:(c + 1) * YB, :HALF]
                    sim = sens[s, b, c * YB:(c + 1) * YB, HALF:]
                    ure = ure + (sre * ire + sim * iim)
                    uim = uim + (sre * iim - sim * ire)
            acc[b, direction, :, :HALF] += cosine * ure + sine * uim
            acc[b, direction, :, HALF:] += cosine * uim - sine * ure
        return carry

    lax.fori_loop(0, total, unit, 0)
    out_ref[...] = acc[...].astype(BF)


def gridded(slots, meta, data, sens, traj, coefs, line, basy, basx):
    vm = pl.BlockSpec(memory_space=pltpu.VMEM)
    return pl.pallas_call(
        functools.partial(image_kernel, slots),
        in_specs=[pl.BlockSpec(memory_space=pltpu.SMEM)] + [vm] * 7,
        out_specs=vm,
        out_shape=jax.ShapeDtypeStruct((4, 16, YB, IMG), BF),
        scratch_shapes=[
            pltpu.VMEM((4, 16, YB, IMG), F32),
            pltpu.VMEM((2, 4, 4 * YB, IMG), F32),
            pltpu.VMEM((4, 4 * YB, HALF), BF),
        ],
        compiler_params=pltpu.CompilerParams(vmem_limit_bytes=48 << 20),
        cost_estimate=pl.CostEstimate(flops=2 * slots * 2048 * 256 * 256, bytes_accessed=16 << 20, transcendentals=0),
        name="gridded",
    )(meta, data, sens, traj, coefs, line, basy, basx)


def on_device(kspace, accept, trajectory, phase_coef, sens):
    zh, zl = lax.axis_index("zh"), lax.axis_index("zl")
    x, core = lax.axis_index("x"), lax.axis_index("core")
    half = lax.rem(x, 2)

    kept = accept.reshape(4, 2, 4, 2, SHOTS).transpose(1, 3, 0, 2, 4).reshape(4, 128)
    order = jnp.argsort(1 - kept, axis=1, stable=True)[:, :96]
    counts = jnp.sum(kept, axis=1)
    dir16, shot = order // SHOTS, order % SHOTS
    subset = jnp.arange(4)[:, None]
    direction = (dir16 // 4) * 16 + (subset // 2) * 8 + (dir16 % 4) * 2 + subset % 2
    source = direction * SHOTS + shot
    mine = zl * 2 + core
    meta = jnp.concatenate([lax.dynamic_slice_in_dim(counts, mine, 1, 0), lax.dynamic_index_in_dim(order, mine, 0, False)])

    small = jnp.concatenate(
        [
            lax.dynamic_index_in_dim(trajectory, core, 0, True).astype(F32),
            lax.dynamic_index_in_dim(phase_coef, core, 0, True).reshape(1, SHOTS, PB * PB),
        ],
        2,
    )
    small = lax.all_gather(small, ("zh", "x"), axis=0, tiled=True).reshape(128, 128 + PB * PB)
    coefs = small[:, 128:].reshape(128, PB, PB)
    k = jnp.arange(128)
    part, w, row = k // 64, (k // 16) % 4, k % 4
    wx, wz = w // 2, w % 2
    z = zh * 2 + zl
    picks = []
    for p in range(2):
        rx = jnp.where(wx == x % 2, x, partner(p, x, 4))
        rz = jnp.where(wz == z % 2, z, partner(p, z, 8))
        picks.append((rz * 4 + rx) * 4 + row)
    lines = jnp.concatenate(picks)
    choose = (jnp.arange(128)[:, None] == lines[None, :]).astype(BF)
    traj = jnp.dot(small[:, :128].astype(BF), choose, preferred_element_type=F32).astype(jnp.int32)
    traj = (traj.reshape(128, 2, 128) + IMG * part[None, None, :]).reshape(256, 1, 128)

    basis = basis_const()
    b1, b2, b3 = split3(basis / (2.0 * math.pi))
    basy = jnp.asarray(np.concatenate([b1, b1, b2, b2, b1, b3], 1))
    basx = lax.dynamic_slice_in_dim(jnp.asarray(basis.T.astype(np.float32)), half * HALF, HALF, 1)
    sens_half = jnp.concatenate(
        [
            lax.dynamic_slice_in_dim(sens, half * HALF, HALF, 2),
            lax.dynamic_slice_in_dim(sens, IMG + half * HALF, HALF, 2),
        ],
        2,
    )
    tab, line = readout_const(), line_const()
    flat = kspace.reshape(DIRS * SHOTS, 16, 2 * IMG)

    def run(ident, slots):
        def branch(flat, source, meta, sens_half, traj, coefs, basx):
            index = source[:, : 2 * slots].reshape(4, slots, 2).transpose(0, 2, 1).reshape(-1)
            send = readout(slots, flat, index, tab)
            data, both = exchange(slots, ident, send, sens_half)
            return gridded(slots, meta, data, both, traj, coefs, line, basy, basx)

        return branch

    need = jnp.max(counts)
    level = sum((need > 2 * s).astype(jnp.int32) for s in LEVELS[:-1])
    part_image = lax.switch(level, [run(i, s) for i, s in enumerate(LEVELS)], flat, source, meta, sens_half, traj, coefs, basx)

    rows = lax.all_to_all(part_image, "y", split_axis=0, concat_axis=0, tiled=True)
    rows = jnp.sum(rows.astype(F32), 0).astype(BF)
    rows = rows.reshape(16, 2, 32, IMG).reshape(32, 32, IMG)
    pieces = lax.all_to_all(rows, ("zh", "x", "core"), split_axis=0, concat_axis=0, tiled=True)
    pieces = pieces.reshape(4, 2, 2, 2, 32, 2, HALF).astype(F32)
    total = jnp.sum(pieces, axis=(0, 1))
    return total.transpose(1, 2, 3, 0, 4).reshape(2, 32, 2 * IMG)


def solution(mesh):
    inner = Mesh(mesh.devices.reshape(4, 2, 4, 4, 2), AXES)
    return jax.shard_map(
        on_device,
        mesh=inner,
        in_specs=(
            P(None, None, ("y", "core"), ("zh", "zl", "x"), None),
            P(),
            P(("zh", "zl", "x"), None, None),
            P(("zh", "zl", "x"), None, None, None),
            P(("y", "core"), None, None),
        ),
        out_specs=P(("zh", "zl", "x"), ("y", "core"), None),
        check_vma=False,
    )
```

```python
import functools
import math

import jax
import jax.numpy as jnp
import numpy as np
from jax import lax
from jax.experimental import pallas as pl
from jax.experimental.pallas import tpu as pltpu
from jax.sharding import Mesh, PartitionSpec as P

IMG = 256
SHOTS = 8
PB = 16
DIRS = 64
HALF = IMG // 2
MESH = pl.DeviceIdType.MESH
AXES = ("zh", "zl", "x", "y", "core")
BF = jnp.bfloat16
F32 = jnp.float32

LEVELS = (32, 36, 48)
STEP = {32: 16, 36: 18, 48: 16}


def readout_const():
    k = np.arange(IMG)
    ang = (np.outer(k, k) % IMG).astype(np.float64) * (2.0 * np.pi / IMG)
    c, s = np.cos(ang).astype(np.float32), np.sin(ang).astype(np.float32)
    tab = np.concatenate([np.concatenate([c, s], 1), np.concatenate([-s, c], 1)], 0)
    order = np.concatenate([np.arange(HALF), IMG + np.arange(HALF), HALF + np.arange(HALF), IMG + HALF + np.arange(HALF)])
    return jnp.asarray(tab[:, order]).astype(BF)


def line_const():
    k = np.arange(IMG)
    ang = (np.outer(k, k) % IMG).astype(np.float64) * (2.0 * np.pi / IMG)
    return jnp.asarray(np.concatenate([np.cos(ang), np.sin(ang)], 1).astype(np.float32)).astype(BF)


def basis_const():
    points = np.arange(IMG, dtype=np.float64)
    orders = np.arange(PB, dtype=np.float64)
    return np.cos(np.pi * orders[None, :] * (points[:, None] + 0.5) / IMG)


def split3(a):
    one = np.asarray(a, np.float32).astype(BF)
    rest = np.asarray(a, np.float64) - one.astype(np.float64)
    two = rest.astype(np.float32).astype(BF)
    rest = rest - two.astype(np.float64)
    return one, two, rest.astype(np.float32).astype(BF)


def poly_consts():
    u = np.cos(np.linspace(0, np.pi, 4001)) * 0.125 + 0.125
    t = np.sqrt(np.maximum(u, 0))
    fs = np.where(t > 1e-9, np.sin(2 * np.pi * t) / np.where(t > 1e-9, t, 1), 2 * np.pi)
    return [float(v) for v in np.polyfit(u, fs, 5)], [float(v) for v in np.polyfit(u, np.cos(2 * np.pi * t), 6)]


SIN_C, COS_C = poly_consts()


def sincos_turns(turns):
    t = turns - jnp.round(turns)
    u = t * t
    s = jnp.full_like(u, SIN_C[0])
    for v in SIN_C[1:]:
        s = s * u + v
    c = jnp.full_like(u, COS_C[0])
    for v in COS_C[1:]:
        c = c * u + v
    return s * t, c


def partner(p, i, n):
    if p == 0:
        return i + 1 - 2 * lax.rem(i, 2)
    return lax.rem(i + 2 * lax.rem(i, 2) - 1 + n, n)


def exchange_kernel(slots, idx_ref, tab_ref, small_ref, kspace_ref, sens_ref, recv_ref, both_ref, gath_ref,
                    kv, send, keep_sens, load_sem, send_sem, recv_sem, local_sem):
    zh, zl = lax.axis_index("zh"), lax.axis_index("zl")
    x, y, core = lax.axis_index("x"), lax.axis_index("y"), lax.axis_index("core")
    z = zh * 2 + zl
    half = lax.rem(x, 2)
    src = half * 2 + zl
    count = STEP[slots]

    load = pltpu.make_async_copy(kspace_ref, kv, load_sem)
    load.start()
    load_sens = pltpu.make_async_copy(sens_ref, keep_sens, local_sem.at[2])
    load_sens.start()

    def target(p, bits):
        bx, bz, bc = bits
        tx = partner(p, x, 4) if bx else x
        tz = partner(p, z, 8) if bz else z
        tc = 1 - core if bc else core
        return tz, tx, tc

    def device(p, bits):
        tz, tx, tc = target(p, bits)
        return (tz // 2, lax.rem(tz, 2), tx, y, tc)

    groups = [(bz, bc, p) for bz in (1, 0) for bc in (0, 1) for p in (0, 1)]
    every = [(p, (bx, bz, bc)) for bz, bc, p in groups for bx in (1, 0) if bx + bz + bc]
    spread = [(dz, dx) for dz in range(4) for dx in range(4) if dz + dx]

    def far(shift):
        return (lax.rem(zh + shift[0], 4), zl, lax.rem(x + shift[1], 4), y, core)

    barrier = pltpu.get_barrier_semaphore()
    for p, bits in every:
        pl.semaphore_signal(barrier, inc=1, device_id=device(p, bits), device_id_type=MESH)
    for shift in spread:
        pl.semaphore_signal(barrier, inc=1, device_id=far(shift), device_id_type=MESH)
    pl.semaphore_wait(barrier, len(every) + len(spread))

    copies = []
    n_every = len(every)

    def begin(src_ref, dst_ref, n, where):
        copy = pltpu.make_async_remote_copy(
            src_ref=src_ref, dst_ref=dst_ref, send_sem=send_sem.at[n], recv_sem=recv_sem.at[n],
            device_id=where, device_id_type=MESH,
        )
        copy.start()
        copies.append(copy)

    for n, shift in enumerate(spread):
        begin(small_ref, gath_ref.at[zh * 4 + x], n_every + 1 + n, far(shift))
    locals_ = [pltpu.make_async_copy(small_ref, gath_ref.at[zh * 4 + x], local_sem.at[3])]
    locals_[0].start()
    load_sens.wait()
    begin(keep_sens, both_ref.at[core], n_every, (zh, zl, x, y, 1 - core))
    store = pltpu.make_async_copy(keep_sens, both_ref.at[core], local_sem.at[2])
    store.start()
    locals_.append(store)
    load.wait()

    for g, (bz, bc, p) in enumerate(groups):
        tz, _, tc = target(p, (0, bz, bc))
        base = ((lax.rem(tz, 2) * 2 + tc) * 2 + p) * slots

        def transform(b, carry):
            rows = jnp.concatenate(
                [kv[idx_ref[base + b * count + i]].reshape(16, 2 * IMG) for i in range(count)], 0
            )
            spec = jnp.dot(rows, tab_ref[...], preferred_element_type=F32) * (1.0 / math.sqrt(IMG))
            spec = spec.astype(BF).reshape(count, 16, 2 * IMG)
            send[g, 0, pl.ds(b * count, count)] = spec[:, :, :IMG]
            send[g, 1, pl.ds(b * count, count)] = spec[:, :, IMG:]
            return carry

        lax.fori_loop(0, slots // count, transform, 0)
        for bx in (1, 0):
            column = 1 - half if bx else half
            if bx + bz + bc:
                begin(send.at[g, column], recv_ref.at[p, src, core], every.index((p, (bx, bz, bc))), device(p, (bx, bz, bc)))
            else:
                copy = pltpu.make_async_copy(send.at[g, column], recv_ref.at[p, src, core], local_sem.at[p])
                copy.start()
                locals_.append(copy)
    for copy in locals_:
        copy.wait()
    for copy in copies:
        copy.wait()


def exchange(slots, ident, index, tab, small, kspace, sens):
    any_ = pl.BlockSpec(memory_space=pl.ANY)
    vm = pl.BlockSpec(memory_space=pltpu.VMEM)
    return pl.pallas_call(
        functools.partial(exchange_kernel, slots),
        in_specs=[pl.BlockSpec(memory_space=pltpu.SMEM), vm, vm, any_, any_],
        out_specs=[any_] * 3,
        out_shape=[
            jax.ShapeDtypeStruct((2, 4, 2, slots, 16, IMG), BF),
            jax.ShapeDtypeStruct((2, 4, IMG, IMG), BF),
            jax.ShapeDtypeStruct((16, 24, 128), F32),
        ],
        scratch_shapes=[
            pltpu.VMEM((DIRS * SHOTS, 4, 4, 2 * IMG), BF),
            pltpu.VMEM((8, 2, slots, 16, IMG), BF),
            pltpu.VMEM((4, IMG, IMG), BF),
            pltpu.SemaphoreType.DMA,
            pltpu.SemaphoreType.DMA((30,)),
            pltpu.SemaphoreType.DMA((30,)),
            pltpu.SemaphoreType.DMA((4,)),
        ],
        compiler_params=pltpu.CompilerParams(collective_id=ident, has_side_effects=True, vmem_limit_bytes=40 << 20),
        cost_estimate=pl.CostEstimate(flops=8 * slots * 16 * 512 * 512 * 2, bytes_accessed=16 << 20, transcendentals=0),
        name="exchange",
    )(index, tab, small, kspace, sens)


YB = 64


def image_kernel(slots, meta_ref, data_ref, sens_ref, gath_ref, choose_ref, line_ref, basy_ref, basx_ref, out_ref,
                 acc, sens, weights_a, weights_b, traj, mixes):
    total = meta_ref[0]
    acc[...] = jnp.zeros_like(acc)
    scale = 1.0 / (math.sqrt(128.0) * SHOTS)
    for s in range(2):
        for c in range(4):
            sens[s, :, c * YB:(c + 1) * YB, :] = (sens_ref[s, c].astype(F32) * scale).reshape(4, YB, IMG)

    lines = jnp.dot(gath_ref[:, :8, :].reshape(128, 128).astype(BF), choose_ref[...], preferred_element_type=F32)
    traj[0] = lines[:, :128]
    traj[1] = lines[:, 128:]

    flat = gath_ref[:, 8:, :].reshape(256, 128)
    one = flat.astype(BF)
    rest = flat - one.astype(F32)
    two = rest.astype(BF)
    three = (rest - two.astype(F32)).astype(BF)
    flat6 = jnp.concatenate([one, one, two, two, one, three], 1)
    shot_row = lax.broadcasted_iota(jnp.int32, (128, 128), 0) // PB
    for s in range(SHOTS):
        b1, b2, b3 = [jnp.where(shot_row == s, basx_ref[i].astype(F32), 0.0).astype(BF) for i in range(3)]
        mixes[s] = jnp.dot(flat6, jnp.concatenate([b1, b2, b1, b2, b3, b1], 0), preferred_element_type=F32)

    lane = lax.broadcasted_iota(jnp.int32, (1, HALF), 1)
    coil = lax.rem(lane // 4, 4)
    masks = [jnp.where(coil == c, 1.0, 0.0).astype(BF) for c in range(4)]
    first = lane < 64
    kline = lax.broadcasted_iota(jnp.int32, (IMG, HALF), 0).astype(F32)

    def prepare(j, p, weights):
        code = meta_ref[1 + j]
        pick = jnp.where(kline == traj[p, pl.ds(code, 1), :], 1.0, 0.0).astype(BF)
        cosine = jnp.dot(line_ref[0], pick, preferred_element_type=F32)
        sine = jnp.dot(line_ref[1], pick, preferred_element_type=F32)
        table = jnp.where(first, cosine, sine).astype(BF)
        for c in range(4):
            weights[:, c * YB:(c + 1) * YB, :] = (table * masks[c]).reshape(4, YB, HALF)

    def combine(j, p, slot, weights):
        code = meta_ref[1 + j]
        direction = jnp.where(j < total, code // SHOTS, 16)
        mixed = mixes[lax.rem(code, SHOTS), pl.ds(pl.multiple_of((code // SHOTS) * PB, PB), PB), :]
        one = mixed.astype(BF)
        rest = mixed - one.astype(F32)
        two = rest.astype(BF)
        three = (rest - two.astype(F32)).astype(BF)
        mixed6 = jnp.concatenate([one, two, one, two, three, one], 0)
        rhs = []
        for s in range(2):
            rows = jnp.concatenate([data_ref[p, w, s, slot] for w in range(4)], 0)
            swapped = jnp.concatenate([-rows[:, HALF:], rows[:, :HALF]], 1)
            rhs.append(jnp.concatenate([rows, swapped], 0))
        for b in range(IMG // YB):
            turns = jnp.dot(basy_ref[b * YB:(b + 1) * YB, :], mixed6, preferred_element_type=F32)
            sine, cosine = sincos_turns(turns)
            ure = uim = None
            for s in range(2):
                image = jnp.dot(weights[b], rhs[s], preferred_element_type=F32)
                for c in range(4):
                    ire, iim = image[c * YB:(c + 1) * YB, :HALF], image[c * YB:(c + 1) * YB, HALF:]
                    sre = sens[s, b, c * YB:(c + 1) * YB, :HALF]
                    sim = sens[s, b, c * YB:(c + 1) * YB, HALF:]
                    re = sre * ire + sim * iim
                    im = sre * iim - sim * ire
                    ure = re if ure is None else ure + re
                    uim = im if uim is None else uim + im
            acc[b, direction, :, :HALF] += cosine * ure + sine * uim
            acc[b, direction, :, HALF:] += cosine * uim - sine * ure

    prepare(0, 0, weights_a)

    def pair(i, carry):
        prepare(2 * i + 1, 1, weights_b)
        combine(2 * i, 0, i, weights_a)
        prepare(2 * i + 2, 0, weights_a)
        combine(2 * i + 1, 1, i, weights_b)
        return carry

    lax.fori_loop(0, (total + 1) // 2, pair, 0)
    out_ref[...] = acc[:, :16].astype(BF)


def gridded(slots, meta, data, sens, gath, choose, line, basy, basx):
    vm = pl.BlockSpec(memory_space=pltpu.VMEM)
    return pl.pallas_call(
        functools.partial(image_kernel, slots),
        in_specs=[pl.BlockSpec(memory_space=pltpu.SMEM)] + [vm] * 7,
        out_specs=vm,
        out_shape=jax.ShapeDtypeStruct((4, 16, YB, IMG), BF),
        scratch_shapes=[
            pltpu.VMEM((4, 17, YB, IMG), F32),
            pltpu.VMEM((2, 4, 4 * YB, IMG), F32),
            pltpu.VMEM((4, 4 * YB, HALF), BF),
            pltpu.VMEM((4, 4 * YB, HALF), BF),
            pltpu.VMEM((2, 128, 128), F32),
            pltpu.VMEM((SHOTS, 256, 128), F32),
        ],
        compiler_params=pltpu.CompilerParams(vmem_limit_bytes=48 << 20),
        cost_estimate=pl.CostEstimate(flops=2 * slots * 2048 * 256 * 256, bytes_accessed=16 << 20, transcendentals=0),
        name="gridded",
    )(meta, data, sens, gath, choose, line, basy, basx)


def on_device(kspace, accept, trajectory, phase_coef, sens):
    zh, zl = lax.axis_index("zh"), lax.axis_index("zl")
    x, core = lax.axis_index("x"), lax.axis_index("core")
    half = lax.rem(x, 2)

    kept = accept.reshape(4, 2, 4, 2, SHOTS).transpose(1, 3, 0, 2, 4).reshape(4, 128)
    upto = np.triu(np.ones((128, 128), np.float32))
    place = jnp.dot(kept.astype(F32), jnp.asarray(upto), preferred_element_type=F32).astype(jnp.int32) - 1
    place = jnp.where(kept > 0, place, -1)
    unit = jnp.arange(128, dtype=jnp.int32)
    order = jnp.sum(jnp.where(place[:, None, :] == jnp.arange(96)[None, :, None], unit[None, None, :], 0), 2)
    counts = jnp.sum(kept, axis=1)
    dir16, shot = order // SHOTS, order % SHOTS
    subset = jnp.arange(4)[:, None]
    direction = (dir16 // 4) * 16 + (subset // 2) * 8 + (dir16 % 4) * 2 + subset % 2
    source = direction * SHOTS + shot
    mine = zl * 2 + core
    meta = jnp.concatenate(
        [
            lax.dynamic_slice_in_dim(counts, mine, 1, 0),
            lax.dynamic_index_in_dim(order, mine, 0, False),
            jnp.zeros((7,), jnp.int32),
        ]
    )

    small = jnp.concatenate(
        [
            lax.dynamic_index_in_dim(trajectory, core, 0, False).astype(F32),
            lax.dynamic_index_in_dim(phase_coef, core, 0, False).transpose(1, 0, 2).reshape(PB, SHOTS * PB),
        ],
        0,
    )
    k = jnp.arange(128)
    w, row = (k // 16) % 4, k % 4
    wx, wz = w // 2, w % 2
    z = zh * 2 + zl
    picks = []
    for p in range(2):
        rx = jnp.where(wx == x % 2, x, partner(p, x, 4))
        rz = jnp.where(wz == z % 2, z, partner(p, z, 8))
        picks.append((rz * 4 + rx) * 4 + row)
    choose = (jnp.arange(128)[:, None] == jnp.concatenate(picks)[None, :]).astype(BF)

    basis = basis_const()
    b1, b2, b3 = split3(basis / (2.0 * math.pi))
    basy = jnp.asarray(np.concatenate([b1, b1, b2, b2, b1, b3], 1))
    basx = jnp.asarray(np.stack([np.tile(np.asarray(part).T, (SHOTS, 1)) for part in split3(basis)]))
    basx = lax.dynamic_slice_in_dim(basx, half * HALF, HALF, 2)
    sens_half = jnp.concatenate(
        [
            lax.dynamic_slice_in_dim(sens, half * HALF, HALF, 2),
            lax.dynamic_slice_in_dim(sens, IMG + half * HALF, HALF, 2),
        ],
        2,
    )
    tab = readout_const()
    line = jnp.stack(jnp.split(line_const(), 2, 1))
    flat = kspace.reshape(DIRS * SHOTS, 4, 4, 2 * IMG)

    def run(ident, slots):
        def branch(flat, source, meta, sens_half, small, choose, basx):
            index = source[:, : 2 * slots].reshape(4, slots, 2).transpose(0, 2, 1).reshape(-1)
            data, both, gath = exchange(slots, ident, index, tab, small, flat, sens_half)
            return gridded(slots, meta, data, both, gath, choose, line, basy, basx)

        return branch

    need = jnp.max(counts)
    level = sum((need > 2 * s).astype(jnp.int32) for s in LEVELS[:-1])
    part_image = lax.switch(level, [run(i, s) for i, s in enumerate(LEVELS)], flat, source, meta, sens_half, small, choose, basx)

    rows = lax.all_to_all(part_image, "y", split_axis=0, concat_axis=0, tiled=True)
    rows = jnp.sum(rows.astype(F32), 0).astype(BF)
    rows = rows.reshape(16, 2, 32, IMG).reshape(32, 32, IMG)
    pieces = lax.all_to_all(rows, ("zh", "x", "core"), split_axis=0, concat_axis=0, tiled=True)
    pieces = pieces.reshape(4, 2, 2, 2, 32, 2, HALF).astype(F32)
    total = jnp.sum(pieces, axis=(0, 1))
    return total.transpose(1, 2, 3, 0, 4).reshape(2, 32, 2 * IMG)


def solution(mesh):
    inner = Mesh(mesh.devices.reshape(4, 2, 4, 4, 2), AXES)
    return jax.shard_map(
        on_device,
        mesh=inner,
        in_specs=(
            P(None, None, ("y", "core"), ("zh", "zl", "x"), None),
            P(),
            P(("zh", "zl", "x"), None, None),
            P(("zh", "zl", "x"), None, None, None),
            P(("y", "core"), None, None),
        ),
        out_specs=P(("zh", "zl", "x"), ("y", "core"), None),
        check_vma=False,
    )
```

```python
import functools
import math

import jax
import jax.numpy as jnp
import numpy as np
from jax import lax
from jax.experimental import pallas as pl
from jax.experimental.pallas import tpu as pltpu
from jax.sharding import Mesh, PartitionSpec as P

IMG = 256
SHOTS = 8
PB = 16
DIRS = 64
HALF = IMG // 2
MESH = pl.DeviceIdType.MESH
AXES = ("zh", "zl", "x", "y", "core")
BF = jnp.bfloat16
F32 = jnp.float32

LEVELS = (32, 36, 48)
STEP = {32: 16, 36: 18, 48: 16}


def readout_const():
    k = np.arange(IMG)
    ang = (np.outer(k, k) % IMG).astype(np.float64) * (2.0 * np.pi / IMG)
    c, s = np.cos(ang).astype(np.float32), np.sin(ang).astype(np.float32)
    tab = np.concatenate([np.concatenate([c, s], 1), np.concatenate([-s, c], 1)], 0)
    order = np.concatenate([np.arange(HALF), IMG + np.arange(HALF), HALF + np.arange(HALF), IMG + HALF + np.arange(HALF)])
    return jnp.asarray(tab[:, order]).astype(BF)


def line_const():
    k = np.arange(IMG)
    ang = (np.outer(k, k) % IMG).astype(np.float64) * (2.0 * np.pi / IMG)
    return jnp.asarray(np.concatenate([np.cos(ang), np.sin(ang)], 1).astype(np.float32)).astype(BF)


def basis_const():
    points = np.arange(IMG, dtype=np.float64)
    orders = np.arange(PB, dtype=np.float64)
    return np.cos(np.pi * orders[None, :] * (points[:, None] + 0.5) / IMG)


def split3(a):
    one = np.asarray(a, np.float32).astype(BF)
    rest = np.asarray(a, np.float64) - one.astype(np.float64)
    two = rest.astype(np.float32).astype(BF)
    rest = rest - two.astype(np.float64)
    return one, two, rest.astype(np.float32).astype(BF)


def poly_consts():
    u = np.cos(np.linspace(0, np.pi, 4001)) * 0.125 + 0.125
    t = np.sqrt(np.maximum(u, 0))
    fs = np.where(t > 1e-9, np.sin(2 * np.pi * t) / np.where(t > 1e-9, t, 1), 2 * np.pi)
    return [float(v) for v in np.polyfit(u, fs, 5)], [float(v) for v in np.polyfit(u, np.cos(2 * np.pi * t), 6)]


SIN_C, COS_C = poly_consts()


def sincos_turns(turns):
    t = turns - jnp.round(turns)
    u = t * t
    s = jnp.full_like(u, SIN_C[0])
    for v in SIN_C[1:]:
        s = s * u + v
    c = jnp.full_like(u, COS_C[0])
    for v in COS_C[1:]:
        c = c * u + v
    return s * t, c


def partner(p, i, n):
    if p == 0:
        return i + 1 - 2 * lax.rem(i, 2)
    return lax.rem(i + 2 * lax.rem(i, 2) - 1 + n, n)


def exchange_kernel(slots, idx_ref, tab_ref, small_ref, kspace_ref, sens_ref, recv_ref, both_ref, gath_ref,
                    kv, send, keep_sens, load_sem, send_sem, recv_sem, local_sem):
    zh, zl = lax.axis_index("zh"), lax.axis_index("zl")
    x, y, core = lax.axis_index("x"), lax.axis_index("y"), lax.axis_index("core")
    z = zh * 2 + zl
    half = lax.rem(x, 2)
    src = half * 2 + zl
    count = STEP[slots]

    load = pltpu.make_async_copy(kspace_ref, kv, load_sem)
    load.start()
    load_sens = pltpu.make_async_copy(sens_ref, keep_sens, local_sem.at[2])
    load_sens.start()

    def target(p, bits):
        bx, bz, bc = bits
        tx = partner(p, x, 4) if bx else x
        tz = partner(p, z, 8) if bz else z
        tc = 1 - core if bc else core
        return tz, tx, tc

    def device(p, bits):
        tz, tx, tc = target(p, bits)
        return (tz // 2, lax.rem(tz, 2), tx, y, tc)

    groups = [(bz, bc, p) for bz in (1, 0) for bc in (0, 1) for p in (0, 1)]
    every = [(p, (bx, bz, bc)) for bz, bc, p in groups for bx in (1, 0) if bx + bz + bc]
    spread = [(dz, dx) for dz in range(4) for dx in range(4) if dz + dx]

    def far(shift):
        return (lax.rem(zh + shift[0], 4), zl, lax.rem(x + shift[1], 4), y, core)

    barrier = pltpu.get_barrier_semaphore()
    for p, bits in every:
        pl.semaphore_signal(barrier, inc=1, device_id=device(p, bits), device_id_type=MESH)
    for shift in spread:
        pl.semaphore_signal(barrier, inc=1, device_id=far(shift), device_id_type=MESH)
    pl.semaphore_wait(barrier, len(every) + len(spread))

    copies = []
    n_every = len(every)

    def begin(src_ref, dst_ref, n, where):
        copy = pltpu.make_async_remote_copy(
            src_ref=src_ref, dst_ref=dst_ref, send_sem=send_sem.at[n], recv_sem=recv_sem.at[n],
            device_id=where, device_id_type=MESH,
        )
        copy.start()
        copies.append(copy)

    for n, shift in enumerate(spread):
        begin(small_ref, gath_ref.at[lax.rem(x - zh + 4, 4) * 4 + zh], n_every + 1 + n, far(shift))
    locals_ = [pltpu.make_async_copy(small_ref, gath_ref.at[lax.rem(x - zh + 4, 4) * 4 + zh], local_sem.at[3])]
    locals_[0].start()
    load_sens.wait()
    begin(keep_sens, both_ref.at[core], n_every, (zh, zl, x, y, 1 - core))
    store = pltpu.make_async_copy(keep_sens, both_ref.at[core], local_sem.at[2])
    store.start()
    locals_.append(store)
    load.wait()

    for g, (bz, bc, p) in enumerate(groups):
        tz, _, tc = target(p, (0, bz, bc))
        base = ((lax.rem(tz, 2) * 2 + tc) * 2 + p) * slots

        def transform(b, carry):
            rows = jnp.concatenate(
                [kv[idx_ref[base + b * count + i]].reshape(16, 2 * IMG) for i in range(count)], 0
            )
            spec = jnp.dot(rows, tab_ref[...], preferred_element_type=F32) * (1.0 / math.sqrt(IMG))
            spec = spec.astype(BF).reshape(count, 16, 2 * IMG)
            send[g, 0, pl.ds(b * count, count)] = spec[:, :, :IMG]
            send[g, 1, pl.ds(b * count, count)] = spec[:, :, IMG:]
            return carry

        lax.fori_loop(0, slots // count, transform, 0)
        for bx in (1, 0):
            column = 1 - half if bx else half
            if bx + bz + bc:
                begin(send.at[g, column], recv_ref.at[p, src, core], every.index((p, (bx, bz, bc))), device(p, (bx, bz, bc)))
            else:
                copy = pltpu.make_async_copy(send.at[g, column], recv_ref.at[p, src, core], local_sem.at[p])
                copy.start()
                locals_.append(copy)
    for copy in locals_:
        copy.wait()
    for copy in copies:
        copy.wait()


def exchange(slots, ident, index, tab, small, kspace, sens):
    any_ = pl.BlockSpec(memory_space=pl.ANY)
    vm = pl.BlockSpec(memory_space=pltpu.VMEM)
    return pl.pallas_call(
        functools.partial(exchange_kernel, slots),
        in_specs=[pl.BlockSpec(memory_space=pltpu.SMEM), vm, vm, any_, any_],
        out_specs=[any_] * 3,
        out_shape=[
            jax.ShapeDtypeStruct((2, 4, 2, slots, 16, IMG), BF),
            jax.ShapeDtypeStruct((2, 4, IMG, IMG), BF),
            jax.ShapeDtypeStruct((16, 24, 128), F32),
        ],
        scratch_shapes=[
            pltpu.VMEM((DIRS * SHOTS, 4, 4, 2 * IMG), BF),
            pltpu.VMEM((8, 2, slots, 16, IMG), BF),
            pltpu.VMEM((4, IMG, IMG), BF),
            pltpu.SemaphoreType.DMA,
            pltpu.SemaphoreType.DMA((30,)),
            pltpu.SemaphoreType.DMA((30,)),
            pltpu.SemaphoreType.DMA((4,)),
        ],
        compiler_params=pltpu.CompilerParams(collective_id=ident, has_side_effects=True, vmem_limit_bytes=40 << 20),
        cost_estimate=pl.CostEstimate(flops=8 * slots * 16 * 512 * 512 * 2, bytes_accessed=16 << 20, transcendentals=0),
        name="exchange",
    )(index, tab, small, kspace, sens)


YB = 64


def image_kernel(slots, meta_ref, data_ref, sens_ref, gath_ref, choose_ref, line_ref, basy_ref, basx_ref, out_ref,
                 acc, sens, weights_a, weights_b, traj, mixes):
    total = meta_ref[0]
    acc[...] = jnp.zeros_like(acc)
    scale = 1.0 / (math.sqrt(128.0) * SHOTS)
    for s in range(2):
        for c in range(4):
            sens[s, :, c * YB:(c + 1) * YB, :] = (sens_ref[s, c].astype(F32) * scale).reshape(4, YB, IMG)

    lines = jnp.dot(gath_ref[:, :8, :].reshape(128, 128).astype(BF), choose_ref[...], preferred_element_type=F32)
    traj[0] = lines[:, :128]
    traj[1] = lines[:, 128:]

    flat = gath_ref[:, 8:, :].reshape(256, 128)
    one = flat.astype(BF)
    rest = flat - one.astype(F32)
    two = rest.astype(BF)
    three = (rest - two.astype(F32)).astype(BF)
    flat6 = jnp.concatenate([one, one, two, two, one, three], 1)
    shot_row = lax.broadcasted_iota(jnp.int32, (128, 128), 0) // PB
    for s in range(SHOTS):
        b1, b2, b3 = [jnp.where(shot_row == s, basx_ref[i].astype(F32), 0.0).astype(BF) for i in range(3)]
        mixes[s] = jnp.dot(flat6, jnp.concatenate([b1, b2, b1, b2, b3, b1], 0), preferred_element_type=F32)

    lane = lax.broadcasted_iota(jnp.int32, (1, HALF), 1)
    coil = lax.rem(lane // 4, 4)
    masks = [jnp.where(coil == c, 1.0, 0.0).astype(BF) for c in range(4)]
    first = lane < 64
    kline = lax.broadcasted_iota(jnp.int32, (IMG, HALF), 0).astype(F32)

    def prepare(j, p, weights):
        code = meta_ref[1 + j]
        pick = jnp.where(kline == traj[p, pl.ds(code, 1), :], 1.0, 0.0).astype(BF)
        cosine = jnp.dot(line_ref[0], pick, preferred_element_type=F32)
        sine = jnp.dot(line_ref[1], pick, preferred_element_type=F32)
        table = jnp.where(first, cosine, sine).astype(BF)
        for c in range(4):
            weights[:, c * YB:(c + 1) * YB, :] = (table * masks[c]).reshape(4, YB, HALF)

    def combine(j, p, slot, weights):
        code = meta_ref[1 + j]
        direction = jnp.where(j < total, code // SHOTS, 16)
        mixed = mixes[lax.rem(code, SHOTS), pl.ds(pl.multiple_of((code // SHOTS) * PB, PB), PB), :]
        one = mixed.astype(BF)
        rest = mixed - one.astype(F32)
        two = rest.astype(BF)
        three = (rest - two.astype(F32)).astype(BF)
        mixed6 = jnp.concatenate([one, two, one, two, three, one], 0)
        rhs = []
        for s in range(2):
            rows = jnp.concatenate([data_ref[p, w, s, slot] for w in range(4)], 0)
            swapped = jnp.concatenate([-rows[:, HALF:], rows[:, :HALF]], 1)
            rhs.append(jnp.concatenate([rows, swapped], 0))
        for b in range(IMG // YB):
            turns = jnp.dot(basy_ref[b * YB:(b + 1) * YB, :], mixed6, preferred_element_type=F32)
            sine, cosine = sincos_turns(turns)
            ure = uim = None
            for s in range(2):
                image = jnp.dot(weights[b], rhs[s], preferred_element_type=F32)
                for c in range(4):
                    ire, iim = image[c * YB:(c + 1) * YB, :HALF], image[c * YB:(c + 1) * YB, HALF:]
                    sre = sens[s, b, c * YB:(c + 1) * YB, :HALF]
                    sim = sens[s, b, c * YB:(c + 1) * YB, HALF:]
                    re = sre * ire + sim * iim
                    im = sre * iim - sim * ire
                    ure = re if ure is None else ure + re
                    uim = im if uim is None else uim + im
            acc[b, direction, :, :HALF] += cosine * ure + sine * uim
            acc[b, direction, :, HALF:] += cosine * uim - sine * ure

    prepare(0, 0, weights_a)

    def pair(i, carry):
        prepare(2 * i + 1, 1, weights_b)
        combine(2 * i, 0, i, weights_a)
        prepare(2 * i + 2, 0, weights_a)
        combine(2 * i + 1, 1, i, weights_b)
        return carry

    lax.fori_loop(0, (total + 1) // 2, pair, 0)
    out_ref[...] = acc[:, :16].astype(BF)


def gridded(slots, meta, data, sens, gath, choose, line, basy, basx):
    vm = pl.BlockSpec(memory_space=pltpu.VMEM)
    return pl.pallas_call(
        functools.partial(image_kernel, slots),
        in_specs=[pl.BlockSpec(memory_space=pltpu.SMEM)] + [vm] * 7,
        out_specs=vm,
        out_shape=jax.ShapeDtypeStruct((4, 16, YB, IMG), BF),
        scratch_shapes=[
            pltpu.VMEM((4, 17, YB, IMG), F32),
            pltpu.VMEM((2, 4, 4 * YB, IMG), F32),
            pltpu.VMEM((4, 4 * YB, HALF), BF),
            pltpu.VMEM((4, 4 * YB, HALF), BF),
            pltpu.VMEM((2, 128, 128), F32),
            pltpu.VMEM((SHOTS, 256, 128), F32),
        ],
        compiler_params=pltpu.CompilerParams(vmem_limit_bytes=48 << 20),
        cost_estimate=pl.CostEstimate(flops=2 * slots * 2048 * 256 * 256, bytes_accessed=16 << 20, transcendentals=0),
        name="gridded",
    )(meta, data, sens, gath, choose, line, basy, basx)


def reduce_kernel(part_ref, out_ref, yr, zs, zr, ysend, yrecv, zsend, zrecv):
    zh, zl = lax.axis_index("zh"), lax.axis_index("zl")
    x, y, core = lax.axis_index("x"), lax.axis_index("y"), lax.axis_index("core")

    def along(r):
        return (zh, zl, x, lax.rem(y + r, 4), core)

    def away(dz, dx, dc):
        return (lax.rem(zh + dz, 4), zl, lax.rem(x + dx, 4), y, 1 - core if dc else core)

    shifts = [(dz, (dz + t) % 4, dc) for t in range(4) for dz in range(4) for dc in range(2)]
    barrier = pltpu.get_barrier_semaphore()
    for r in (1, 2, 3):
        pl.semaphore_signal(barrier, inc=1, device_id=along(r), device_id_type=MESH)
    for shift in shifts[1:]:
        pl.semaphore_signal(barrier, inc=1, device_id=away(*shift), device_id_type=MESH)
    pl.semaphore_wait(barrier, 34)

    def group(t):
        return lax.rem(x - zh + t + 4, 4)

    rows = []
    for t in range(4):
        for r in (2, 1, 3):
            copy = pltpu.make_async_remote_copy(
                src_ref=part_ref.at[lax.rem(y + r, 4), pl.ds(group(t) * 4, 4)],
                dst_ref=yr.at[t, r - 1],
                send_sem=ysend.at[t, r - 1],
                recv_sem=yrecv.at[t, r - 1],
                device_id=along(r),
                device_id_type=MESH,
            )
            copy.start()
            rows.append(copy)
    pieces = []
    for t in range(4):
        for copy in rows[3 * t:3 * t + 3]:
            copy.wait_recv()
        for dz in range(4):
            there = lax.rem(zh + dz, 4)
            total = part_ref[y, group(t) * 4 + there].astype(F32)
            for r in range(3):
                total = total + yr[t, r, there].astype(F32)
            for dc in range(2):
                n = (t * 4 + dz) * 2 + dc
                zs[n * 2:n * 2 + 2] = total.astype(BF).reshape(2, 32, IMG)
                to = 1 - core if dc else core
                if n:
                    copy = pltpu.make_async_remote_copy(
                        src_ref=zs.at[n * 2 + to],
                        dst_ref=zr.at[n],
                        send_sem=zsend.at[n],
                        recv_sem=zrecv.at[n],
                        device_id=away(dz, (dz + t) % 4, dc),
                        device_id_type=MESH,
                    )
                    copy.start()
                    pieces.append(copy)
                else:
                    zr[0] = zs[to]
    for copy in pieces:
        copy.wait_recv()
    for dc in range(2):
        e = 1 - core if dc else core
        for odd in range(2):
            half = lax.rem(x + odd, 2)
            total = None
            for n, (dz, dx, c) in enumerate(shifts):
                if c == dc and dx % 2 == odd:
                    total = zr[n].astype(F32) if total is None else total + zr[n].astype(F32)
            out_ref[e, :, pl.ds(pl.multiple_of(half * HALF, HALF), HALF)] = total[:, :HALF]
            out_ref[e, :, pl.ds(pl.multiple_of(IMG + half * HALF, HALF), HALF)] = total[:, HALF:]
    for copy in rows + pieces:
        copy.wait_send()


def reduced(part):
    vm = pl.BlockSpec(memory_space=pltpu.VMEM)
    return pl.pallas_call(
        reduce_kernel,
        in_specs=[vm],
        out_specs=vm,
        out_shape=jax.ShapeDtypeStruct((2, 32, 2 * IMG), F32),
        scratch_shapes=[
            pltpu.VMEM((4, 3, 4, YB, IMG), BF),
            pltpu.VMEM((64, 32, IMG), BF),
            pltpu.VMEM((32, 32, IMG), BF),
            pltpu.SemaphoreType.DMA((4, 3)),
            pltpu.SemaphoreType.DMA((4, 3)),
            pltpu.SemaphoreType.DMA((32,)),
            pltpu.SemaphoreType.DMA((32,)),
        ],
        compiler_params=pltpu.CompilerParams(collective_id=8, has_side_effects=True),
        name="reduced",
    )(part)


def on_device(kspace, accept, trajectory, phase_coef, sens):
    zh, zl = lax.axis_index("zh"), lax.axis_index("zl")
    x, core = lax.axis_index("x"), lax.axis_index("core")
    half = lax.rem(x, 2)

    owner_zh, owner_x = np.arange(16) % 4, (np.arange(16) // 4 + np.arange(16)) % 4
    listed = np.stack([owner_zh * 16 + (q // 2) * 8 + owner_x * 2 + q % 2 for q in range(4)]).astype(np.int32)
    choice = (listed.reshape(-1)[:, None] == np.arange(DIRS)[None, :]).astype(np.float32)
    kept = jnp.dot(jnp.asarray(choice), accept.astype(F32)).astype(jnp.int32).reshape(4, 128)
    upto = np.triu(np.ones((128, 128), np.float32))
    place = jnp.dot(kept.astype(F32), jnp.asarray(upto), preferred_element_type=F32).astype(jnp.int32) - 1
    place = jnp.where(kept > 0, place, -1)
    unit = jnp.arange(128, dtype=jnp.int32)
    order = jnp.sum(jnp.where(place[:, None, :] == jnp.arange(96)[None, :, None], unit[None, None, :], 0), 2)
    counts = jnp.sum(kept, axis=1)
    dir16, shot = order // SHOTS, order % SHOTS
    subset = jnp.arange(4)[:, None]
    direction = (dir16 % 4) * 16 + (subset // 2) * 8 + ((dir16 // 4 + dir16) % 4) * 2 + subset % 2
    source = direction * SHOTS + shot
    mine = zl * 2 + core
    meta = jnp.concatenate(
        [
            lax.dynamic_slice_in_dim(counts, mine, 1, 0),
            lax.dynamic_index_in_dim(order, mine, 0, False),
            jnp.zeros((7,), jnp.int32),
        ]
    )

    small = jnp.concatenate(
        [
            lax.dynamic_index_in_dim(trajectory, core, 0, False).astype(F32),
            lax.dynamic_index_in_dim(phase_coef, core, 0, False).transpose(1, 0, 2).reshape(PB, SHOTS * PB),
        ],
        0,
    )
    k = jnp.arange(128)
    w, row = (k // 16) % 4, k % 4
    wx, wz = w // 2, w % 2
    z = zh * 2 + zl
    picks = []
    for p in range(2):
        rx = jnp.where(wx == x % 2, x, partner(p, x, 4))
        rz = jnp.where(wz == z % 2, z, partner(p, z, 8))
        picks.append((rz * 4 + rx) * 4 + row)
    choose = (jnp.arange(128)[:, None] == jnp.concatenate(picks)[None, :]).astype(BF)

    basis = basis_const()
    b1, b2, b3 = split3(basis / (2.0 * math.pi))
    basy = jnp.asarray(np.concatenate([b1, b1, b2, b2, b1, b3], 1))
    basx = jnp.asarray(np.stack([np.tile(np.asarray(part).T, (SHOTS, 1)) for part in split3(basis)]))
    basx = lax.dynamic_slice_in_dim(basx, half * HALF, HALF, 2)
    sens_half = jnp.concatenate(
        [
            lax.dynamic_slice_in_dim(sens, half * HALF, HALF, 2),
            lax.dynamic_slice_in_dim(sens, IMG + half * HALF, HALF, 2),
        ],
        2,
    )
    tab = readout_const()
    line = jnp.stack(jnp.split(line_const(), 2, 1))
    flat = kspace.reshape(DIRS * SHOTS, 4, 4, 2 * IMG)

    def run(ident, slots):
        def branch(flat, source, meta, sens_half, small, choose, basx):
            index = source[:, : 2 * slots].reshape(4, slots, 2).transpose(0, 2, 1).reshape(-1)
            data, both, gath = exchange(slots, ident, index, tab, small, flat, sens_half)
            return gridded(slots, meta, data, both, gath, choose, line, basy, basx)

        return branch

    need = jnp.max(counts)
    level = sum((need > 2 * s).astype(jnp.int32) for s in LEVELS[:-1])
    part_image = lax.switch(level, [run(i, s) for i, s in enumerate(LEVELS)], flat, source, meta, sens_half, small, choose, basx)

    return reduced(part_image)


def solution(mesh):
    inner = Mesh(mesh.devices.reshape(4, 2, 4, 4, 2), AXES)
    return jax.shard_map(
        on_device,
        mesh=inner,
        in_specs=(
            P(None, None, ("y", "core"), ("zh", "zl", "x"), None),
            P(),
            P(("zh", "zl", "x"), None, None),
            P(("zh", "zl", "x"), None, None, None),
            P(("y", "core"), None, None),
        ),
        out_specs=P(("zh", "zl", "x"), ("y", "core"), None),
        check_vma=False,
    )
```

```python
import functools
import math

import jax
import jax.numpy as jnp
import numpy as np
from jax import lax
from jax.experimental import pallas as pl
from jax.experimental.pallas import tpu as pltpu
from jax.sharding import Mesh, PartitionSpec as P

IMG = 256
SHOTS = 8
PB = 16
DIRS = 64
HALF = IMG // 2
MESH = pl.DeviceIdType.MESH
AXES = ("zh", "zl", "x", "y", "core")
BF = jnp.bfloat16
F32 = jnp.float32

LEVELS = (32, 36, 48)
CHUNKS = 4
YB = 64


def readout_const():
    k = np.arange(IMG)
    ang = (np.outer(k, k) % IMG).astype(np.float64) * (2.0 * np.pi / IMG)
    c, s = np.cos(ang).astype(np.float32), np.sin(ang).astype(np.float32)
    tab = np.concatenate([np.concatenate([c, s], 1), np.concatenate([-s, c], 1)], 0)
    order = np.concatenate([np.arange(HALF), IMG + np.arange(HALF), HALF + np.arange(HALF), IMG + HALF + np.arange(HALF)])
    return jnp.asarray(tab[:, order]).astype(BF)


def line_const():
    k = np.arange(IMG)
    ang = (np.outer(k, k) % IMG).astype(np.float64) * (2.0 * np.pi / IMG)
    return jnp.asarray(np.concatenate([np.cos(ang), np.sin(ang)], 1).astype(np.float32)).astype(BF)


def basis_const():
    points = np.arange(IMG, dtype=np.float64)
    orders = np.arange(PB, dtype=np.float64)
    return np.cos(np.pi * orders[None, :] * (points[:, None] + 0.5) / IMG)


def split3(a):
    one = np.asarray(a, np.float32).astype(BF)
    rest = np.asarray(a, np.float64) - one.astype(np.float64)
    two = rest.astype(np.float32).astype(BF)
    rest = rest - two.astype(np.float64)
    return one, two, rest.astype(np.float32).astype(BF)


def poly_consts():
    u = np.cos(np.linspace(0, np.pi, 4001)) * 0.125 + 0.125
    t = np.sqrt(np.maximum(u, 0))
    fs = np.where(t > 1e-9, np.sin(2 * np.pi * t) / np.where(t > 1e-9, t, 1), 2 * np.pi)
    return [float(v) for v in np.polyfit(u, fs, 5)], [float(v) for v in np.polyfit(u, np.cos(2 * np.pi * t), 6)]


SIN_C, COS_C = poly_consts()


def sincos_turns(turns):
    t = turns - jnp.round(turns)
    u = t * t
    s = jnp.full_like(u, SIN_C[0])
    for v in SIN_C[1:]:
        s = s * u + v
    c = jnp.full_like(u, COS_C[0])
    for v in COS_C[1:]:
        c = c * u + v
    return s * t, c


def partner(p, i, n):
    if p == 0:
        return i + 1 - 2 * lax.rem(i, 2)
    return lax.rem(i + 2 * lax.rem(i, 2) - 1 + n, n)


def split_bf16(a):
    one = a.astype(BF)
    rest = a - one.astype(F32)
    two = rest.astype(BF)
    return one, two, (rest - two.astype(F32)).astype(BF)


def kernel(slots, idx_ref, meta_ref, take_ref, weight_ref, tab_ref, small_ref, choose_ref, line_ref, basy_ref, basx_ref, kspace_ref,
           sens_ref, out_ref, kv, send, recv, both, gath, contrib, sens, weights_a, weights_b, traj, mixes, relay_out,
           relay_in, block_out, block_in, zs, zr, load_sem, local_sem, self_sem, send_sem, recv_sem, spread_send, spread_recv,
           relay_sems, block_sems, zsend, zrecv):
    zh, zl = lax.axis_index("zh"), lax.axis_index("zl")
    x, y, core = lax.axis_index("x"), lax.axis_index("y"), lax.axis_index("core")
    z = zh * 2 + zl
    half = lax.rem(x, 2)
    src = half * 2 + zl
    part = slots // CHUNKS

    load = pltpu.make_async_copy(kspace_ref, kv, load_sem)
    load.start()
    own_sens = pltpu.make_async_copy(sens_ref, both.at[core], local_sem.at[0])
    own_sens.start()

    def target(p, bits):
        bx, bz, bc = bits
        tx = partner(p, x, 4) if bx else x
        tz = partner(p, z, 8) if bz else z
        tc = 1 - core if bc else core
        return tz // 2, lax.rem(tz, 2), tx, y, tc

    def far(dz, dx, dc=0):
        return (lax.rem(zh + dz, 4), zl, lax.rem(x + dx, 4), y, 1 - core if dc else core)

    def along(r):
        return (zh, zl, x, lax.rem(y + r, 4), core)

    groups = [(bz, bc, p) for bz in (1, 0) for bc in (0, 1) for p in (0, 1)]
    every = [(g, p, (bx, bz, bc)) for g, (bz, bc, p) in enumerate(groups) for bx in (1, 0) if bx + bz + bc]
    spread = [(dz, dx) for dz in range(4) for dx in range(4) if dz + dx]
    shifts = [(dz, (dz + t) % 4, dc) for t in range(4) for dz in range(4) for dc in range(2)]
    core_peer = (zh, zl, x, y, 1 - core)

    barrier = pltpu.get_barrier_semaphore()
    for _, p, bits in every:
        pl.semaphore_signal(barrier, inc=1, device_id=target(p, bits), device_id_type=MESH)
    for shift in shifts[1:]:
        pl.semaphore_signal(barrier, inc=1, device_id=far(*shift), device_id_type=MESH)
    for r in (1, 3):
        pl.semaphore_signal(barrier, inc=1, device_id=along(r), device_id_type=MESH)
    pl.semaphore_wait(barrier, len(every) + len(shifts) - 1 + 2)

    def remote(src_ref, dst_ref, sems, n, where):
        return pltpu.make_async_remote_copy(
            src_ref=src_ref, dst_ref=dst_ref, send_sem=sems[0].at[n], recv_sem=sems[1].at[n],
            device_id=where, device_id_type=MESH,
        )

    place = lax.rem(x - zh + 4, 4) * 4 + zh
    spread_sems = (spread_send, spread_recv)
    first_copies = [remote(small_ref, gath.at[place], spread_sems, n, far(*shift)) for n, shift in enumerate(spread)]
    first_copies.append(remote(sens_ref, both.at[core], spread_sems, len(spread), core_peer))
    for copy in first_copies:
        copy.start()
    gath[place] = small_ref[...]

    def piece(c):
        return pl.ds(c * part, part)

    def chunk_copy(c, n):
        g, p, bits = every[n]
        column = 1 - half if bits[0] else half
        return pltpu.make_async_remote_copy(
            src_ref=send.at[g, column, piece(c)], dst_ref=recv.at[p, src, core, piece(c)],
            send_sem=send_sem.at[n, c], recv_sem=recv_sem.at[n, c], device_id=target(p, bits), device_id_type=MESH,
        )

    def self_copy(c, p):
        return pltpu.make_async_copy(send.at[4 + p, half, piece(c)], recv.at[p, src, core, piece(c)], self_sem.at[p, c])

    load.wait()

    def transform(c, carry):
        def one_group(g, carry):
            zb, cb = lax.rem(zl + 1 - g // 4, 2), lax.rem(core + lax.rem(g // 2, 2), 2)
            base = ((zb * 2 + cb) * 2 + lax.rem(g, 2)) * slots + c * part
            rows = jnp.concatenate([kv[idx_ref[base + i]].reshape(16, 2 * IMG) for i in range(part)], 0)
            spec = jnp.dot(rows, tab_ref[...], preferred_element_type=F32) * (1.0 / math.sqrt(IMG))
            spec = spec.astype(BF).reshape(part, 16, 2 * IMG)
            send[g, 0, piece(c)] = spec[:, :, :IMG]
            send[g, 1, piece(c)] = spec[:, :, IMG:]
            return carry

        lax.fori_loop(0, 8, one_group, 0)
        for n in range(len(every)):
            chunk_copy(c, n).start()
        for p in range(2):
            self_copy(c, p).start()
        return carry

    lax.fori_loop(0, CHUNKS, transform, 0)

    own_sens.wait()
    for copy in first_copies:
        copy.wait()
    scale = 1.0 / (math.sqrt(128.0) * SHOTS)
    for s in range(2):
        for c in range(4):
            sens[s, :, c * YB:(c + 1) * YB, :] = (both[s, c].astype(F32) * scale).reshape(4, YB, IMG)
    lines = jnp.dot(gath[:, :8, :].reshape(128, 128).astype(BF), choose_ref[...], preferred_element_type=F32)
    traj[0:128] = lines[:, :128].reshape(128, 1, 128)
    traj[128:256] = lines[:, 128:].reshape(128, 1, 128)
    one, two, three = split_bf16(gath[:, 8:, :].reshape(256, 128))
    flat6 = jnp.concatenate([one, one, two, two, one, three], 1)
    shot_row = lax.broadcasted_iota(jnp.int32, (128, 128), 0) // PB
    for s in range(SHOTS):
        b1, b2, b3 = [jnp.where(shot_row == s, basx_ref[i].astype(F32), 0.0).astype(BF) for i in range(3)]
        mixed = jnp.dot(flat6, jnp.concatenate([b1, b2, b1, b2, b3, b1], 0), preferred_element_type=F32)
        mixes[16 * s:16 * s + 16] = mixed.reshape(16, PB, 128)

    lane = lax.broadcasted_iota(jnp.int32, (1, HALF), 1)
    coil = lax.rem(lane // 4, 4)
    masks = [jnp.where(coil == c, 1.0, 0.0).astype(BF) for c in range(4)]
    first = lane < 64
    kline = lax.broadcasted_iota(jnp.int32, (IMG, HALF), 0).astype(F32)

    def prepare(j, p, weights):
        pick = jnp.where(kline == traj[meta_ref[j]], 1.0, 0.0).astype(BF)
        cosine = jnp.dot(line_ref[0], pick, preferred_element_type=F32)
        sine = jnp.dot(line_ref[1], pick, preferred_element_type=F32)
        table = jnp.where(first, cosine, sine).astype(BF)
        for c in range(4):
            weights[:, c * YB:(c + 1) * YB, :] = (table * masks[c]).reshape(4, YB, HALF)

    def combine(j, p, slot, weights):
        one, two, three = split_bf16(mixes[meta_ref[104 + j]])
        mixed6 = jnp.concatenate([one, two, one, two, three, one], 0)
        rhs = []
        for s in range(2):
            rows = jnp.concatenate([recv[p, w, s, slot] for w in range(4)], 0)
            swapped = jnp.concatenate([-rows[:, HALF:], rows[:, :HALF]], 1)
            rhs.append(jnp.concatenate([rows, swapped], 0))
        for b in range(IMG // YB):
            turns = jnp.dot(basy_ref[b * YB:(b + 1) * YB, :], mixed6, preferred_element_type=F32)
            sine, cosine = sincos_turns(turns)
            ure = uim = None
            for s in range(2):
                image = jnp.dot(weights[b], rhs[s], preferred_element_type=F32)
                for c in range(4):
                    ire, iim = image[c * YB:(c + 1) * YB, :HALF], image[c * YB:(c + 1) * YB, HALF:]
                    sre = sens[s, b, c * YB:(c + 1) * YB, :HALF]
                    sim = sens[s, b, c * YB:(c + 1) * YB, HALF:]
                    re = sre * ire + sim * iim
                    im = sre * iim - sim * ire
                    ure = re if ure is None else ure + re
                    uim = im if uim is None else uim + im
            contrib[j, b, :, :HALF] = cosine * ure + sine * uim
            contrib[j, b, :, HALF:] = cosine * uim - sine * ure

    prepare(0, 0, weights_a)

    def work(c, carry):
        for n in range(len(every)):
            chunk_copy(c, n).wait_recv()
        for p in range(2):
            self_copy(c, p).wait()

        def pair(k, carry):
            i = c * part + k
            prepare(2 * i + 1, 1, weights_b)
            combine(2 * i, 0, i, weights_a)
            prepare(2 * i + 2, 0, weights_a)
            combine(2 * i + 1, 1, i, weights_b)
            return carry

        lax.fori_loop(0, part, pair, 0)
        return carry

    lax.fori_loop(0, CHUNKS, work, 0)

    def shots(o, b):
        total = None
        for s in range(6):
            term = contrib[take_ref[o * 6 + s], b] * weight_ref[o * 6 + s]
            total = term if total is None else total + term
        return total

    def group(t):
        return lax.rem(x - zh + t + 4, 4) * 4

    ring = ((1, 0), (3, 2))
    relays, blocks, pieces = [], [], []
    for t in range(4):
        for way, (r, k0) in enumerate(ring):
            for k in range(2):
                relay_out[t, way, k] = shots(group(t) + k0 + k, lax.rem(y + 2, 4)).astype(BF)
            copy = remote(relay_out.at[t, way], relay_in.at[t, way], relay_sems, t * 2 + way, along(r))
            copy.start()
            relays.append(copy)
    for t in range(4):
        for way, (r, k0) in enumerate(ring):
            there = lax.rem(y + r, 4)
            relays[t * 2 + way].wait_recv()
            for k in range(4):
                total = shots(group(t) + k, there)
                if k0 <= k < k0 + 2:
                    total = total + relay_in[t, way, k - k0].astype(F32)
                block_out[t, way, k] = total.astype(BF)
            copy = remote(block_out.at[t, way], block_in.at[t, way], block_sems, t * 2 + way, along(r))
            copy.start()
            blocks.append(copy)
    for t in range(4):
        blocks[t * 2].wait_recv()
        blocks[t * 2 + 1].wait_recv()
        for dz in range(4):
            there = lax.rem(zh + dz, 4)
            total = shots(group(t) + there, y) + block_in[t, 0, there].astype(F32) + block_in[t, 1, there].astype(F32)
            for dc in range(2):
                n = (t * 4 + dz) * 2 + dc
                zs[n * 2:n * 2 + 2] = total.astype(BF).reshape(2, 32, IMG)
                to = 1 - core if dc else core
                if n:
                    copy = remote(zs.at[n * 2 + to], zr.at[n], (zsend, zrecv), n, far(dz, (dz + t) % 4, dc))
                    copy.start()
                    pieces.append(copy)
                else:
                    zr[0] = zs[to]
    for copy in pieces:
        copy.wait_recv()
    for dc in range(2):
        e = 1 - core if dc else core
        for odd in range(2):
            column = lax.rem(x + odd, 2)
            total = None
            for n, (dz, dx, c) in enumerate(shifts):
                if c == dc and dx % 2 == odd:
                    total = zr[n].astype(F32) if total is None else total + zr[n].astype(F32)
            out_ref[e, :, pl.ds(pl.multiple_of(column * HALF, HALF), HALF)] = total[:, :HALF]
            out_ref[e, :, pl.ds(pl.multiple_of(IMG + column * HALF, HALF), HALF)] = total[:, HALF:]
    for copy in relays + blocks + pieces:
        copy.wait_send()

    def sent(c, carry):
        for n in range(len(every)):
            chunk_copy(c, n).wait_send()
        return carry

    lax.fori_loop(0, CHUNKS, sent, 0)


def combined(slots, ident, index, meta, take, weight, tab, small, choose, line, basy, basx, kspace, sens):
    any_ = pl.BlockSpec(memory_space=pl.ANY)
    vm = pl.BlockSpec(memory_space=pltpu.VMEM)
    sm = pl.BlockSpec(memory_space=pltpu.SMEM)
    dma = pltpu.SemaphoreType.DMA
    return pl.pallas_call(
        functools.partial(kernel, slots),
        in_specs=[sm, sm, sm, sm] + [vm] * 6 + [any_, any_],
        out_specs=vm,
        out_shape=jax.ShapeDtypeStruct((2, 32, 2 * IMG), F32),
        scratch_shapes=[
            pltpu.VMEM((DIRS * SHOTS, 4, 4, 2 * IMG), BF),
            pltpu.VMEM((8, 2, slots, 16, IMG), BF),
            pltpu.VMEM((2, 4, 2, slots, 16, IMG), BF),
            pltpu.VMEM((2, 4, IMG, IMG), BF),
            pltpu.VMEM((16, 24, 128), F32),
            pltpu.VMEM((2 * slots, 4, YB, IMG), F32),
            pltpu.VMEM((2, 4, 4 * YB, IMG), F32),
            pltpu.VMEM((4, 4 * YB, HALF), BF),
            pltpu.VMEM((4, 4 * YB, HALF), BF),
            pltpu.VMEM((256, 1, 128), F32),
            pltpu.VMEM((128, PB, 128), F32),
            pltpu.VMEM((4, 2, 2, YB, IMG), BF),
            pltpu.VMEM((4, 2, 2, YB, IMG), BF),
            pltpu.VMEM((4, 2, 4, YB, IMG), BF),
            pltpu.VMEM((4, 2, 4, YB, IMG), BF),
            pltpu.VMEM((64, 32, IMG), BF),
            pltpu.VMEM((32, 32, IMG), BF),
            dma,
            dma((1,)),
            dma((2, CHUNKS)),
            dma((14, CHUNKS)),
            dma((14, CHUNKS)),
            dma((16,)),
            dma((16,)),
            [dma((8,)), dma((8,))],
            [dma((8,)), dma((8,))],
            dma((32,)),
            dma((32,)),
        ],
        compiler_params=pltpu.CompilerParams(collective_id=ident, has_side_effects=True, vmem_limit_bytes=67000000),
        cost_estimate=pl.CostEstimate(flops=2 * slots * 4096 * 256 * 256, bytes_accessed=16 << 20, transcendentals=0),
        name="combined",
    )(index, meta, take, weight, tab, small, choose, line, basy, basx, kspace, sens)


def on_device(kspace, accept, trajectory, phase_coef, sens):
    zh, zl = lax.axis_index("zh"), lax.axis_index("zl")
    x, core = lax.axis_index("x"), lax.axis_index("core")
    half = lax.rem(x, 2)

    owner_zh, owner_x = np.arange(16) % 4, (np.arange(16) // 4 + np.arange(16)) % 4
    listed = np.stack([owner_zh * 16 + (q // 2) * 8 + owner_x * 2 + q % 2 for q in range(4)]).astype(np.int32)
    choice = (listed.reshape(-1)[:, None] == np.arange(DIRS)[None, :]).astype(np.float32)
    kept = jnp.dot(jnp.asarray(choice), accept.astype(F32)).astype(jnp.int32).reshape(4, 128)
    upto = np.triu(np.ones((128, 128), np.float32))
    upto_count = jnp.dot(kept.astype(F32), jnp.asarray(upto), preferred_element_type=F32).astype(jnp.int32)
    place = jnp.where(kept > 0, upto_count - 1, -1)
    unit = jnp.arange(128, dtype=jnp.int32)
    order = jnp.sum(jnp.where(place[:, None, :] == jnp.arange(96)[None, :, None], unit[None, None, :], 0), 2)
    counts = jnp.sum(kept, axis=1)
    dir16, shot = order // SHOTS, order % SHOTS
    subset = jnp.arange(4)[:, None]
    direction = (dir16 % 4) * 16 + (subset // 2) * 8 + ((dir16 // 4 + dir16) % 4) * 2 + subset % 2
    source = direction * SHOTS + shot
    mine = zl * 2 + core
    kept16 = lax.dynamic_index_in_dim(kept, mine, 0, False).reshape(16, SHOTS)
    starts = lax.dynamic_index_in_dim(upto_count, mine, 0, False).reshape(16, SHOTS)[:, 0] - kept16[:, 0]
    codes = jnp.concatenate([lax.dynamic_index_in_dim(order, mine, 0, False), jnp.zeros((8,), jnp.int32)])
    meta = jnp.concatenate([codes + 128 * (jnp.arange(104) % 2), (codes % SHOTS) * 16 + codes // SHOTS])
    take = (starts[:, None] + jnp.arange(6)[None, :]).reshape(96)
    weight = (jnp.arange(6)[None, :] < jnp.sum(kept16, 1, keepdims=True)).astype(F32).reshape(96)

    small = jnp.concatenate(
        [
            lax.dynamic_index_in_dim(trajectory, core, 0, False).astype(F32),
            lax.dynamic_index_in_dim(phase_coef, core, 0, False).transpose(1, 0, 2).reshape(PB, SHOTS * PB),
        ],
        0,
    )
    k = jnp.arange(128)
    w, row = (k // 16) % 4, k % 4
    wx, wz = w // 2, w % 2
    z = zh * 2 + zl
    picks = []
    for p in range(2):
        rx = jnp.where(wx == x % 2, x, partner(p, x, 4))
        rz = jnp.where(wz == z % 2, z, partner(p, z, 8))
        picks.append((rz * 4 + rx) * 4 + row)
    choose = (jnp.arange(128)[:, None] == jnp.concatenate(picks)[None, :]).astype(BF)

    basis = basis_const()
    b1, b2, b3 = split3(basis / (2.0 * math.pi))
    basy = jnp.asarray(np.concatenate([b1, b1, b2, b2, b1, b3], 1))
    basx = jnp.asarray(np.stack([np.tile(np.asarray(part).T, (SHOTS, 1)) for part in split3(basis)]))
    basx = lax.dynamic_slice_in_dim(basx, half * HALF, HALF, 2)
    sens_half = jnp.concatenate(
        [
            lax.dynamic_slice_in_dim(sens, half * HALF, HALF, 2),
            lax.dynamic_slice_in_dim(sens, IMG + half * HALF, HALF, 2),
        ],
        2,
    )
    tab = readout_const()
    line = jnp.stack(jnp.split(line_const(), 2, 1))
    flat = kspace.reshape(DIRS * SHOTS, 4, 4, 2 * IMG)

    def run(ident, slots):
        def branch(flat, source, meta, take, weight, sens_half, small, choose, basx):
            take = jnp.minimum(take, 2 * slots - 1)
            index = source[:, : 2 * slots].reshape(4, slots, 2).transpose(0, 2, 1).reshape(-1)
            return combined(slots, ident, index, meta, take, weight, tab, small, choose, line, basy, basx, flat, sens_half)

        return branch

    need = jnp.max(counts)
    level = sum((need > 2 * s).astype(jnp.int32) for s in LEVELS[:-1])
    return lax.switch(
        level, [run(i, s) for i, s in enumerate(LEVELS)], flat, source, meta, take, weight, sens_half, small, choose, basx
    )


def solution(mesh):
    inner = Mesh(mesh.devices.reshape(4, 2, 4, 4, 2), AXES)
    return jax.shard_map(
        on_device,
        mesh=inner,
        in_specs=(
            P(None, None, ("y", "core"), ("zh", "zl", "x"), None),
            P(),
            P(("zh", "zl", "x"), None, None),
            P(("zh", "zl", "x"), None, None, None),
            P(("y", "core"), None, None),
        ),
        out_specs=P(("zh", "zl", "x"), ("y", "core"), None),
        check_vma=False,
    )
```

```python
import functools
import math

import jax
import jax.numpy as jnp
import numpy as np
from jax import lax
from jax.experimental import pallas as pl
from jax.experimental.pallas import tpu as pltpu
from jax.sharding import Mesh, PartitionSpec as P

IMG = 256
SHOTS = 8
PB = 16
DIRS = 64
HALF = IMG // 2
MESH = pl.DeviceIdType.MESH
AXES = ("zh", "zl", "x", "y", "core")
BF = jnp.bfloat16
F32 = jnp.float32

LEVELS = (32, 36, 48)
CHUNKS = 4
YB = 64


def readout_const():
    k = np.arange(IMG)
    ang = (np.outer(k, k) % IMG).astype(np.float64) * (2.0 * np.pi / IMG)
    c, s = np.cos(ang).astype(np.float32), np.sin(ang).astype(np.float32)
    tab = np.concatenate([np.concatenate([c, s], 1), np.concatenate([-s, c], 1)], 0)
    order = np.concatenate([np.arange(HALF), IMG + np.arange(HALF), HALF + np.arange(HALF), IMG + HALF + np.arange(HALF)])
    return jnp.asarray(tab[:, order]).astype(BF)


def line_const():
    k = np.arange(IMG)
    ang = (np.outer(k, k) % IMG).astype(np.float64) * (2.0 * np.pi / IMG)
    return jnp.asarray(np.concatenate([np.cos(ang), np.sin(ang)], 1).astype(np.float32)).astype(BF)


def basis_const():
    points = np.arange(IMG, dtype=np.float64)
    orders = np.arange(PB, dtype=np.float64)
    return np.cos(np.pi * orders[None, :] * (points[:, None] + 0.5) / IMG)


def split3(a):
    one = np.asarray(a, np.float32).astype(BF)
    rest = np.asarray(a, np.float64) - one.astype(np.float64)
    two = rest.astype(np.float32).astype(BF)
    rest = rest - two.astype(np.float64)
    return one, two, rest.astype(np.float32).astype(BF)


def poly_consts():
    u = np.cos(np.linspace(0, np.pi, 4001)) * 0.125 + 0.125
    t = np.sqrt(np.maximum(u, 0))
    fs = np.where(t > 1e-9, np.sin(2 * np.pi * t) / np.where(t > 1e-9, t, 1), 2 * np.pi)
    return [float(v) for v in np.polyfit(u, fs, 5)], [float(v) for v in np.polyfit(u, np.cos(2 * np.pi * t), 6)]


SIN_C, COS_C = poly_consts()


def sincos_turns(turns):
    t = turns - jnp.round(turns)
    u = t * t
    s = jnp.full_like(u, SIN_C[0])
    for v in SIN_C[1:]:
        s = s * u + v
    c = jnp.full_like(u, COS_C[0])
    for v in COS_C[1:]:
        c = c * u + v
    return s * t, c


def partner(p, i, n):
    if p == 0:
        return i + 1 - 2 * lax.rem(i, 2)
    return lax.rem(i + 2 * lax.rem(i, 2) - 1 + n, n)


def split_bf16(a):
    one = a.astype(BF)
    rest = a - one.astype(F32)
    two = rest.astype(BF)
    return one, two, (rest - two.astype(F32)).astype(BF)


def kernel(slots, plan_ref, traj_ref, coef_ref, tab_ref, line_ref, basy_ref, basx_ref, kspace_ref, sens_ref, out_ref, small, kv, send, recv, both, gath, contrib, sens, weights_a, weights_b, traj, mixes, relay_out,
           relay_in, block_out, block_in, zs, zr, load_sem, local_sem, self_sem, send_sem, recv_sem, spread_send, spread_recv,
           relay_sems, block_sems, zsend, zrecv):
    zh, zl = lax.axis_index("zh"), lax.axis_index("zl")
    x, y, core = lax.axis_index("x"), lax.axis_index("y"), lax.axis_index("core")
    z = zh * 2 + zl
    half = lax.rem(x, 2)
    src = half * 2 + zl
    part = slots // CHUNKS

    load = pltpu.make_async_copy(kspace_ref, kv, load_sem)
    load.start()
    sens_parts = [
        (sens_ref.at[:, :, pl.ds(pl.multiple_of(k * IMG + half * HALF, HALF), HALF)], both.at[core, :, :, k * HALF:(k + 1) * HALF])
        for k in range(2)
    ]
    own_sens = [pltpu.make_async_copy(a, b, local_sem.at[k]) for k, (a, b) in enumerate(sens_parts)]
    for copy in own_sens:
        copy.start()

    def target(p, bits):
        bx, bz, bc = bits
        tx = partner(p, x, 4) if bx else x
        tz = partner(p, z, 8) if bz else z
        tc = 1 - core if bc else core
        return tz // 2, lax.rem(tz, 2), tx, y, tc

    def far(dz, dx, dc=0):
        return (lax.rem(zh + dz, 4), zl, lax.rem(x + dx, 4), y, 1 - core if dc else core)

    def along(r):
        return (zh, zl, x, lax.rem(y + r, 4), core)

    groups = [(bz, bc, p) for bz in (1, 0) for bc in (0, 1) for p in (0, 1)]
    every = [(g, p, (bx, bz, bc)) for g, (bz, bc, p) in enumerate(groups) for bx in (1, 0) if bx + bz + bc]
    turn = [(bx, bz, bc, p) for bc in (0, 1) for bx, bz in ((1, 1), (0, 1), (1, 0)) for p in (0, 1)] + [(0, 0, 1, 0), (0, 0, 1, 1)]
    order = [[(b[0], b[1], b[2], p) for _, p, b in every].index(entry) for entry in turn]
    spread = [(dz, dx) for dz in range(4) for dx in range(4) if dz + dx]
    shifts = [(dz, (dz + t) % 4, dc) for t in range(4) for dz in range(4) for dc in range(2)]
    core_peer = (zh, zl, x, y, 1 - core)

    small[0:SHOTS] = traj_ref[core].astype(F32)
    term = lax.broadcasted_iota(jnp.int32, (PB, 128), 0)
    place_lane = lax.broadcasted_iota(jnp.int32, (PB, 128), 1)
    spread_out = None
    for s in range(SHOTS):
        where = (place_lane == s * PB + term).astype(F32)
        moved = jnp.dot(coef_ref[core, s], where, preferred_element_type=F32, precision=lax.Precision.HIGHEST)
        spread_out = moved if spread_out is None else spread_out + moved
    small[SHOTS:] = spread_out

    barrier = pltpu.get_barrier_semaphore()
    for _, p, bits in every:
        pl.semaphore_signal(barrier, inc=1, device_id=target(p, bits), device_id_type=MESH)
    for shift in shifts[1:]:
        pl.semaphore_signal(barrier, inc=1, device_id=far(*shift), device_id_type=MESH)
    for r in (1, 3):
        pl.semaphore_signal(barrier, inc=1, device_id=along(r), device_id_type=MESH)
    pl.semaphore_wait(barrier, len(every) + len(shifts) - 1 + 2)

    def remote(src_ref, dst_ref, sems, n, where):
        return pltpu.make_async_remote_copy(
            src_ref=src_ref, dst_ref=dst_ref, send_sem=sems[0].at[n], recv_sem=sems[1].at[n],
            device_id=where, device_id_type=MESH,
        )

    place = lax.rem(x - zh + 4, 4) * 4 + zh
    spread_sems = (spread_send, spread_recv)
    first_copies = [remote(small, gath.at[place], spread_sems, n, far(*shift)) for n, shift in enumerate(spread)]
    for k, (a, b) in enumerate(sens_parts):
        first_copies.append(remote(a, b, spread_sems, len(spread) + k, core_peer))
    for copy in first_copies:
        copy.start()
    gath[place] = small[...]

    def piece(c):
        return pl.ds(c * part, part)

    def chunk_copy(c, n):
        g, p, bits = every[n]
        column = 1 - half if bits[0] else half
        return pltpu.make_async_remote_copy(
            src_ref=send.at[g, column, piece(c)], dst_ref=recv.at[p, src, core, piece(c)],
            send_sem=send_sem.at[n, c], recv_sem=recv_sem.at[n, c], device_id=target(p, bits), device_id_type=MESH,
        )

    def self_copy(c, p):
        return pltpu.make_async_copy(send.at[4 + p, half, piece(c)], recv.at[p, src, core, piece(c)], self_sem.at[p, c])

    load.wait()

    def transform(c, carry):
        def one_group(g, carry):
            zb, cb = lax.rem(zl + 1 - g // 4, 2), lax.rem(core + lax.rem(g // 2, 2), 2)
            base = c * part * 2 + lax.rem(g, 2)
            rows = jnp.concatenate([kv[plan_ref[zb * 2 + cb, base + 2 * i]].reshape(16, 2 * IMG) for i in range(part)], 0)
            spec = jnp.dot(rows, tab_ref[...], preferred_element_type=F32) * (1.0 / math.sqrt(IMG))
            spec = spec.astype(BF).reshape(part, 16, 2 * IMG)
            send[g, 0, piece(c)] = spec[:, :, :IMG]
            send[g, 1, piece(c)] = spec[:, :, IMG:]
            return carry

        lax.fori_loop(0, 8, one_group, 0)
        for n in order:
            chunk_copy(c, n).start()
        for p in range(2):
            self_copy(c, p).start()
        return carry

    lax.fori_loop(0, CHUNKS, transform, 0)

    for copy in own_sens:
        copy.wait()
    for copy in first_copies:
        copy.wait()
    scale = 1.0 / (math.sqrt(128.0) * SHOTS)
    for s in range(2):
        for c in range(4):
            sens[s, :, c * YB:(c + 1) * YB, :] = (both[s, c].astype(F32) * scale).reshape(4, YB, IMG)
    k = lax.broadcasted_iota(jnp.int32, (1, 128), 1)
    wx, wz = lax.rem(k // 32, 2), lax.rem(k // 16, 2)
    line_numbers = gath[:, :SHOTS, :].reshape(128, 128).astype(BF)
    for p in range(2):
        rx = jnp.where(wx == half, x, partner(p, x, 4))
        rz = jnp.where(wz == zl, z, partner(p, z, 8))
        wanted = (rz * 4 + rx) * 4 + lax.rem(k, 4)
        choose = (lax.broadcasted_iota(jnp.int32, (128, 128), 0) == wanted).astype(F32).astype(BF)
        lines = jnp.dot(line_numbers, choose, preferred_element_type=F32)
        traj[128 * p:128 * p + 128] = lines.reshape(128, 1, 128)
    one, two, three = split_bf16(gath[:, SHOTS:, :].reshape(256, 128))
    flat6 = jnp.concatenate([one, one, two, two, one, three], 1)
    shot_row = lax.broadcasted_iota(jnp.int32, (128, 128), 0) // PB
    columns = pl.ds(pl.multiple_of(half * HALF, HALF), HALF)
    for s in range(SHOTS):
        b1, b2, b3 = [jnp.where(shot_row == s, basx_ref[i, :, columns].astype(F32), 0.0).astype(BF) for i in range(3)]
        mixed = jnp.dot(flat6, jnp.concatenate([b1, b2, b1, b2, b3, b1], 0), preferred_element_type=F32)
        mixes[16 * s:16 * s + 16] = mixed.reshape(16, PB, 128)

    lane = lax.broadcasted_iota(jnp.int32, (1, HALF), 1)
    coil = lax.rem(lane // 4, 4)
    masks = [jnp.where(coil == c, 1.0, 0.0).astype(BF) for c in range(4)]
    first = lane < 64
    kline = lax.broadcasted_iota(jnp.int32, (IMG, HALF), 0).astype(F32)

    def prepare(j, p, weights):
        pick = jnp.where(kline == traj[plan_ref[4, j]], 1.0, 0.0).astype(BF)
        cosine = jnp.dot(line_ref[0], pick, preferred_element_type=F32)
        sine = jnp.dot(line_ref[1], pick, preferred_element_type=F32)
        table = jnp.where(first, cosine, sine).astype(BF)
        for c in range(4):
            weights[:, c * YB:(c + 1) * YB, :] = (table * masks[c]).reshape(4, YB, HALF)

    def combine(j, p, slot, weights):
        one, two, three = split_bf16(mixes[plan_ref[5, j]])
        mixed6 = jnp.concatenate([one, two, one, two, three, one], 0)
        rhs = []
        for s in range(2):
            rows = jnp.concatenate([recv[p, w, s, slot] for w in range(4)], 0)
            swapped = jnp.concatenate([-rows[:, HALF:], rows[:, :HALF]], 1)
            rhs.append(jnp.concatenate([rows, swapped], 0))
        for b in range(IMG // YB):
            turns = jnp.dot(basy_ref[b * YB:(b + 1) * YB, :], mixed6, preferred_element_type=F32)
            sine, cosine = sincos_turns(turns)
            ure = uim = None
            for s in range(2):
                image = jnp.dot(weights[b], rhs[s], preferred_element_type=F32)
                for c in range(4):
                    ire, iim = image[c * YB:(c + 1) * YB, :HALF], image[c * YB:(c + 1) * YB, HALF:]
                    sre = sens[s, b, c * YB:(c + 1) * YB, :HALF]
                    sim = sens[s, b, c * YB:(c + 1) * YB, HALF:]
                    re = sre * ire + sim * iim
                    im = sre * iim - sim * ire
                    ure = re if ure is None else ure + re
                    uim = im if uim is None else uim + im
            contrib[j, b, :, :HALF] = cosine * ure + sine * uim
            contrib[j, b, :, HALF:] = cosine * uim - sine * ure

    prepare(0, 0, weights_a)

    def work(c, carry):
        for n in range(len(every)):
            chunk_copy(c, n).wait_recv()
        for p in range(2):
            self_copy(c, p).wait()

        def pair(k, carry):
            i = c * part + k
            prepare(2 * i + 1, 1, weights_b)
            combine(2 * i, 0, i, weights_a)
            prepare(2 * i + 2, 0, weights_a)
            combine(2 * i + 1, 1, i, weights_b)
            return carry

        lax.fori_loop(0, part, pair, 0)
        return carry

    lax.fori_loop(0, CHUNKS, work, 0)

    def shots(o, b):
        total = None
        for s in range(6):
            term = contrib[plan_ref[6, o * SHOTS + s], b] * plan_ref[7, o * SHOTS + s].astype(F32)
            total = term if total is None else total + term
        return total

    def group(t):
        return lax.rem(x - zh + t + 4, 4) * 4

    ring = ((1, 0), (3, 2))
    relays, blocks, pieces = [], [], []
    for t in range(4):
        for way, (r, k0) in enumerate(ring):
            for k in range(2):
                relay_out[t, way, k] = shots(group(t) + k0 + k, lax.rem(y + 2, 4)).astype(BF)
            copy = remote(relay_out.at[t, way], relay_in.at[t, way], relay_sems, t * 2 + way, along(r))
            copy.start()
            relays.append(copy)
    for t in range(4):
        for way, (r, k0) in enumerate(ring):
            there = lax.rem(y + r, 4)
            relays[t * 2 + way].wait_recv()
            for k in range(4):
                total = shots(group(t) + k, there)
                if k0 <= k < k0 + 2:
                    total = total + relay_in[t, way, k - k0].astype(F32)
                block_out[t, way, k] = total.astype(BF)
            copy = remote(block_out.at[t, way], block_in.at[t, way], block_sems, t * 2 + way, along(r))
            copy.start()
            blocks.append(copy)
    for t in range(4):
        blocks[t * 2].wait_recv()
        blocks[t * 2 + 1].wait_recv()
        for dz in range(4):
            there = lax.rem(zh + dz, 4)
            total = shots(group(t) + there, y) + block_in[t, 0, there].astype(F32) + block_in[t, 1, there].astype(F32)
            for dc in range(2):
                n = (t * 4 + dz) * 2 + dc
                zs[n * 2:n * 2 + 2] = total.astype(BF).reshape(2, 32, IMG)
                to = 1 - core if dc else core
                if n:
                    copy = remote(zs.at[n * 2 + to], zr.at[n], (zsend, zrecv), n, far(dz, (dz + t) % 4, dc))
                    copy.start()
                    pieces.append(copy)
                else:
                    zr[0] = zs[to]
    for copy in pieces:
        copy.wait_recv()
    for dc in range(2):
        e = 1 - core if dc else core
        for odd in range(2):
            column = lax.rem(x + odd, 2)
            total = None
            for n, (dz, dx, c) in enumerate(shifts):
                if c == dc and dx % 2 == odd:
                    total = zr[n].astype(F32) if total is None else total + zr[n].astype(F32)
            out_ref[e, :, pl.ds(pl.multiple_of(column * HALF, HALF), HALF)] = total[:, :HALF]
            out_ref[e, :, pl.ds(pl.multiple_of(IMG + column * HALF, HALF), HALF)] = total[:, HALF:]
    for copy in relays + blocks + pieces:
        copy.wait_send()

    def sent(c, carry):
        for n in range(len(every)):
            chunk_copy(c, n).wait_send()
        return carry

    lax.fori_loop(0, CHUNKS, sent, 0)


def combined(slots, ident, plan, traj, coefs, tab, line, basy, basx, kspace, sens):
    any_ = pl.BlockSpec(memory_space=pl.ANY)
    vm = pl.BlockSpec(memory_space=pltpu.VMEM)
    sm = pl.BlockSpec(memory_space=pltpu.SMEM)
    dma = pltpu.SemaphoreType.DMA
    return pl.pallas_call(
        functools.partial(kernel, slots),
        in_specs=[sm] + [vm] * 6 + [any_, any_],
        out_specs=vm,
        out_shape=jax.ShapeDtypeStruct((2, 32, 2 * IMG), F32),
        scratch_shapes=[
            pltpu.VMEM((24, 128), F32),
            pltpu.VMEM((DIRS * SHOTS, 4, 4, 2 * IMG), BF),
            pltpu.VMEM((8, 2, slots, 16, IMG), BF),
            pltpu.VMEM((2, 4, 2, slots, 16, IMG), BF),
            pltpu.VMEM((2, 4, IMG, IMG), BF),
            pltpu.VMEM((16, 24, 128), F32),
            pltpu.VMEM((2 * slots, 4, YB, IMG), F32),
            pltpu.VMEM((2, 4, 4 * YB, IMG), F32),
            pltpu.VMEM((4, 4 * YB, HALF), BF),
            pltpu.VMEM((4, 4 * YB, HALF), BF),
            pltpu.VMEM((256, 1, 128), F32),
            pltpu.VMEM((128, PB, 128), F32),
            pltpu.VMEM((4, 2, 2, YB, IMG), BF),
            pltpu.VMEM((4, 2, 2, YB, IMG), BF),
            pltpu.VMEM((4, 2, 4, YB, IMG), BF),
            pltpu.VMEM((4, 2, 4, YB, IMG), BF),
            pltpu.VMEM((64, 32, IMG), BF),
            pltpu.VMEM((32, 32, IMG), BF),
            dma,
            dma((2,)),
            dma((2, CHUNKS)),
            dma((14, CHUNKS)),
            dma((14, CHUNKS)),
            dma((17,)),
            dma((17,)),
            [dma((8,)), dma((8,))],
            [dma((8,)), dma((8,))],
            dma((32,)),
            dma((32,)),
        ],
        compiler_params=pltpu.CompilerParams(collective_id=ident, has_side_effects=True, vmem_limit_bytes=67000000),
        cost_estimate=pl.CostEstimate(flops=2 * slots * 4096 * 256 * 256, bytes_accessed=16 << 20, transcendentals=0),
        name="combined",
    )(plan, traj, coefs, tab, line, basy, basx, kspace, sens)


def plan_kernel(accept_ref, plan_ref):
    mine = lax.axis_index("zl") * 2 + lax.axis_index("core")

    def iota(shape, axis):
        return lax.broadcasted_iota(jnp.int32, shape, axis)

    def flag(cond):
        return jnp.where(cond, 1.0, 0.0)

    tile = flag(lax.rem(iota((SHOTS, 128), 1), SHOTS) == iota((SHOTS, 128), 0)).astype(BF)
    flags = jnp.dot(accept_ref[...].astype(F32).astype(BF), tile, preferred_element_type=F32)
    lane = iota((1, 128), 1)
    o, s = lane // SHOTS, lax.rem(lane, SHOTS)
    first = lax.rem(o, 4) * 16 + lax.rem(o // 4 + o, 4) * 2
    row = iota((8, 128), 0)
    kept = jnp.zeros((8, 128), F32)
    for q in range(4):
        listed = iota((DIRS, 128), 0) == first + (q // 2) * 8 + q % 2
        kept = kept + jnp.where(row == q, jnp.sum(jnp.where(listed, flags, 0.0), 0, keepdims=True), 0.0)
    a, b = iota((128, 128), 0), iota((128, 128), 1)
    keptb = kept.astype(BF)
    upto = jnp.dot(keptb, flag(a <= b).astype(BF), preferred_element_type=F32)
    total = jnp.dot(keptb, jnp.ones((128, 128), BF), preferred_element_type=F32)
    count = jnp.dot(keptb, flag(a // SHOTS == b // SHOTS).astype(BF), preferred_element_type=F32)
    begin = jnp.dot((upto - kept).astype(BF), flag(a == b // SHOTS * SHOTS).astype(BF), preferred_element_type=F32)
    place = jnp.where(kept > 0.5, upto - 1.0, -1.0)
    lanef = iota((128, 128), 0).astype(F32)

    def packed(values, where):
        return lax.dot_general(
            values, flag(lanef == where), (((1,), (1,)), ((), ())), preferred_element_type=F32, precision=lax.Precision.HIGHEST
        )

    plan = jnp.zeros((8, 128), F32)
    for q in range(4):
        source = ((first + (q // 2) * 8 + q % 2) * SHOTS + s).astype(F32)
        plan = plan + packed(jnp.where(row == q, source, 0.0), place[q:q + 1])

    def own(v):
        return jnp.sum(jnp.where(row == mine, v, 0.0), 0, keepdims=True)

    codes = jnp.where(row == 4, lane, jnp.where(row == 5, s * 16 + o, 0)).astype(F32)
    plan = plan + packed(codes, own(place))
    plan = plan + jnp.where(row == 4, lax.rem(lane, 2) * 128, 0).astype(F32)
    sf = s.astype(F32)
    take = jnp.minimum(own(begin) + sf, own(total) - 1.0)
    plan = plan + jnp.where(row == 6, take, 0.0) + jnp.where(row == 7, flag(sf < own(count)), 0.0)
    plan_ref[0:8] = plan.astype(jnp.int32)
    plan_ref[8:16] = jnp.broadcast_to(jnp.max(total, 0, keepdims=True), (8, 128)).astype(jnp.int32)


def on_device(kspace, accept, trajectory, phase_coef, sens):
    vm = pl.BlockSpec(memory_space=pltpu.VMEM)
    plan = pl.pallas_call(
        plan_kernel, in_specs=[vm], out_specs=vm, out_shape=jax.ShapeDtypeStruct((16, 128), jnp.int32), name="plan"
    )(accept)

    basis = basis_const()
    b1, b2, b3 = split3(basis / (2.0 * math.pi))
    basy = jnp.asarray(np.concatenate([b1, b1, b2, b2, b1, b3], 1))
    basx = jnp.asarray(np.stack([np.tile(np.asarray(part).T, (SHOTS, 1)) for part in split3(basis)]))
    tab = readout_const()
    line = jnp.stack(jnp.split(line_const(), 2, 1))
    flat = kspace.reshape(DIRS * SHOTS, 4, 4, 2 * IMG)

    def run(ident, slots):
        def branch(flat, plan, trajectory, phase_coef, sens):
            return combined(slots, ident, plan, trajectory, phase_coef, tab, line, basy, basx, flat, sens)

        return branch

    need = plan[8, 0]
    level = sum((need > 2 * s).astype(jnp.int32) for s in LEVELS[:-1])
    return lax.switch(level, [run(i, s) for i, s in enumerate(LEVELS)], flat, plan, trajectory, phase_coef, sens)


def solution(mesh):
    inner = Mesh(mesh.devices.reshape(4, 2, 4, 4, 2), AXES)
    return jax.shard_map(
        on_device,
        mesh=inner,
        in_specs=(
            P(None, None, ("y", "core"), ("zh", "zl", "x"), None),
            P(),
            P(("zh", "zl", "x"), None, None),
            P(("zh", "zl", "x"), None, None, None),
            P(("y", "core"), None, None),
        ),
        out_specs=P(("zh", "zl", "x"), ("y", "core"), None),
        check_vma=False,
    )
```

```python
import functools
import math

import jax
import jax.numpy as jnp
import numpy as np
from jax import lax
from jax.experimental import pallas as pl
from jax.experimental.pallas import tpu as pltpu
from jax.sharding import Mesh, PartitionSpec as P

IMG = 256
SHOTS = 8
PB = 16
DIRS = 64
HALF = IMG // 2
MESH = pl.DeviceIdType.MESH
AXES = ("zh", "zl", "x", "y", "core")
BF = jnp.bfloat16
F32 = jnp.float32

LEVELS = (32, 36, 48)
CHUNKS = 4
YB = 64


def readout_const():
    k = np.arange(IMG)
    ang = (np.outer(k, k) % IMG).astype(np.float64) * (2.0 * np.pi / IMG)
    c, s = np.cos(ang).astype(np.float32), np.sin(ang).astype(np.float32)
    tab = np.concatenate([np.concatenate([c, s], 1), np.concatenate([-s, c], 1)], 0)
    order = np.concatenate([np.arange(HALF), IMG + np.arange(HALF), HALF + np.arange(HALF), IMG + HALF + np.arange(HALF)])
    return jnp.asarray(tab[:, order]).astype(BF)


def line_const():
    k = np.arange(IMG)
    ang = (np.outer(k, k) % IMG).astype(np.float64) * (2.0 * np.pi / IMG)
    return jnp.asarray(np.concatenate([np.cos(ang), np.sin(ang)], 1).astype(np.float32)).astype(BF)


def basis_const():
    points = np.arange(IMG, dtype=np.float64)
    orders = np.arange(PB, dtype=np.float64)
    return np.cos(np.pi * orders[None, :] * (points[:, None] + 0.5) / IMG)


def split3(a):
    one = np.asarray(a, np.float32).astype(BF)
    rest = np.asarray(a, np.float64) - one.astype(np.float64)
    two = rest.astype(np.float32).astype(BF)
    rest = rest - two.astype(np.float64)
    return one, two, rest.astype(np.float32).astype(BF)


def poly_consts():
    u = np.cos(np.linspace(0, np.pi, 4001)) * 0.125 + 0.125
    t = np.sqrt(np.maximum(u, 0))
    fs = np.where(t > 1e-9, np.sin(2 * np.pi * t) / np.where(t > 1e-9, t, 1), 2 * np.pi)
    return [float(v) for v in np.polyfit(u, fs, 5)], [float(v) for v in np.polyfit(u, np.cos(2 * np.pi * t), 6)]


SIN_C, COS_C = poly_consts()


def sincos_turns(turns):
    t = turns - jnp.round(turns)
    u = t * t
    s = jnp.full_like(u, SIN_C[0])
    for v in SIN_C[1:]:
        s = s * u + v
    c = jnp.full_like(u, COS_C[0])
    for v in COS_C[1:]:
        c = c * u + v
    return s * t, c


def partner(p, i, n):
    if p == 0:
        return i + 1 - 2 * lax.rem(i, 2)
    return lax.rem(i + 2 * lax.rem(i, 2) - 1 + n, n)


def split_bf16(a):
    one = a.astype(BF)
    rest = a - one.astype(F32)
    two = rest.astype(BF)
    return one, two, (rest - two.astype(F32)).astype(BF)


def kernel(slots, plan_ref, traj_ref, coef_ref, tab_ref, line_ref, basy_ref, basx_ref, kspace_ref, sens_ref, out_ref, small, kv, send, recv, both, gath, contrib, sens, weights_a, weights_b, traj, mixes, relay_out,
           relay_in, block_out, block_in, zs, zr, load_sem, local_sem, self_sem, send_sem, recv_sem, spread_send, spread_recv,
           relay_sems, block_sems, zsend, zrecv):
    zh, zl = lax.axis_index("zh"), lax.axis_index("zl")
    x, y, core = lax.axis_index("x"), lax.axis_index("y"), lax.axis_index("core")
    z = zh * 2 + zl
    half = lax.rem(x, 2)
    src = half * 2 + zl
    part = slots // CHUNKS

    loads = [
        pltpu.make_async_copy(kspace_ref.at[k * 64:(k + 1) * 64], kv.at[k * 64:(k + 1) * 64], load_sem.at[k]) for k in range(8)
    ]
    for copy in loads:
        copy.start()
    sens_parts = [
        (sens_ref.at[:, :, pl.ds(pl.multiple_of(k * IMG + half * HALF, HALF), HALF)], both.at[core, :, :, k * HALF:(k + 1) * HALF])
        for k in range(2)
    ]
    own_sens = [pltpu.make_async_copy(a, b, local_sem.at[k]) for k, (a, b) in enumerate(sens_parts)]
    for copy in own_sens:
        copy.start()

    def target(p, bits):
        bx, bz, bc = bits
        tx = partner(p, x, 4) if bx else x
        tz = partner(p, z, 8) if bz else z
        tc = 1 - core if bc else core
        return tz // 2, lax.rem(tz, 2), tx, y, tc

    def far(dz, dx, dc=0):
        return (lax.rem(zh + dz, 4), zl, lax.rem(x + dx, 4), y, 1 - core if dc else core)

    def along(r):
        return (zh, zl, x, lax.rem(y + r, 4), core)

    groups = [(bz, bc, p) for bz in (1, 0) for bc in (0, 1) for p in (0, 1)]
    every = [(g, p, (bx, bz, bc)) for g, (bz, bc, p) in enumerate(groups) for bx in (1, 0) if bx + bz + bc]
    turn = [(bx, bz, bc, p) for bc in (0, 1) for bx, bz in ((1, 1), (0, 1), (1, 0)) for p in (0, 1)] + [(0, 0, 1, 0), (0, 0, 1, 1)]
    order = [[(b[0], b[1], b[2], p) for _, p, b in every].index(entry) for entry in turn]
    spread = [(dz, dx) for dz in range(4) for dx in range(4) if dz + dx]
    shifts = [(dz, (dz + t) % 4, dc) for t in range(4) for dz in range(4) for dc in range(2)]
    core_peer = (zh, zl, x, y, 1 - core)

    barrier = pltpu.get_barrier_semaphore()
    for _, p, bits in every:
        pl.semaphore_signal(barrier, inc=1, device_id=target(p, bits), device_id_type=MESH)
    for shift in shifts[1:]:
        pl.semaphore_signal(barrier, inc=1, device_id=far(*shift), device_id_type=MESH)
    for r in (1, 3):
        pl.semaphore_signal(barrier, inc=1, device_id=along(r), device_id_type=MESH)
    small[0:SHOTS] = traj_ref[core].astype(F32)
    term = lax.broadcasted_iota(jnp.int32, (PB, 128), 0)
    place_lane = lax.broadcasted_iota(jnp.int32, (PB, 128), 1)
    spread_out = None
    for s in range(SHOTS):
        where = (place_lane == s * PB + term).astype(F32)
        moved = jnp.dot(coef_ref[core, s], where, preferred_element_type=F32, precision=lax.Precision.HIGHEST)
        spread_out = moved if spread_out is None else spread_out + moved
    small[SHOTS:] = spread_out

    pl.semaphore_wait(barrier, len(every) + len(shifts) - 1 + 2)

    def remote(src_ref, dst_ref, sems, n, where):
        return pltpu.make_async_remote_copy(
            src_ref=src_ref, dst_ref=dst_ref, send_sem=sems[0].at[n], recv_sem=sems[1].at[n],
            device_id=where, device_id_type=MESH,
        )

    place = lax.rem(x - zh + 4, 4) * 4 + zh
    spread_sems = (spread_send, spread_recv)
    first_copies = [remote(small, gath.at[place], spread_sems, n, far(*shift)) for n, shift in enumerate(spread)]
    for k, (a, b) in enumerate(sens_parts):
        first_copies.append(remote(a, b, spread_sems, len(spread) + k, core_peer))
    for copy in first_copies:
        copy.start()
    gath[place] = small[...]

    def piece(c):
        return pl.ds(c * part, part)

    def chunk_copy(c, n):
        g, p, bits = every[n]
        column = 1 - half if bits[0] else half
        return pltpu.make_async_remote_copy(
            src_ref=send.at[g, column, piece(c)], dst_ref=recv.at[p, src, core, piece(c)],
            send_sem=send_sem.at[n, c], recv_sem=recv_sem.at[n, c], device_id=target(p, bits), device_id_type=MESH,
        )

    def self_copy(c, p):
        return pltpu.make_async_copy(send.at[4 + p, half, piece(c)], recv.at[p, src, core, piece(c)], self_sem.at[p, c])

    for copy in loads:
        copy.wait()

    def transform(c, carry):
        def one_group(g, carry):
            zb, cb = lax.rem(zl + 1 - g // 4, 2), lax.rem(core + lax.rem(g // 2, 2), 2)
            base = c * part * 2 + lax.rem(g, 2)
            rows = jnp.concatenate([kv[plan_ref[zb * 2 + cb, base + 2 * i]].reshape(16, 2 * IMG) for i in range(part)], 0)
            spec = jnp.dot(rows, tab_ref[...], preferred_element_type=F32) * (1.0 / math.sqrt(IMG))
            spec = spec.astype(BF).reshape(part, 16, 2 * IMG)
            send[g, 0, piece(c)] = spec[:, :, :IMG]
            send[g, 1, piece(c)] = spec[:, :, IMG:]
            return carry

        lax.fori_loop(0, 8, one_group, 0)
        for n in order:
            chunk_copy(c, n).start()
        for p in range(2):
            self_copy(c, p).start()
        return carry

    lax.fori_loop(0, CHUNKS, transform, 0)

    for copy in own_sens:
        copy.wait()
    for copy in first_copies:
        copy.wait()
    scale = 1.0 / (math.sqrt(128.0) * SHOTS)
    for s in range(2):
        for c in range(4):
            real, imag = both[s, c, :, :HALF].astype(F32) * scale, both[s, c, :, HALF:].astype(F32) * scale
            for k, values in enumerate((real, real - imag, real + imag)):
                sens[s, k, :, c * YB:(c + 1) * YB] = values.reshape(4, YB, HALF)
    k = lax.broadcasted_iota(jnp.int32, (1, 128), 1)
    wx, wz = lax.rem(k // 32, 2), lax.rem(k // 16, 2)
    line_numbers = gath[:, :SHOTS, :].reshape(128, 128).astype(BF)
    for p in range(2):
        rx = jnp.where(wx == half, x, partner(p, x, 4))
        rz = jnp.where(wz == zl, z, partner(p, z, 8))
        wanted = (rz * 4 + rx) * 4 + lax.rem(k, 4)
        choose = (lax.broadcasted_iota(jnp.int32, (128, 128), 0) == wanted).astype(F32).astype(BF)
        lines = jnp.dot(line_numbers, choose, preferred_element_type=F32)
        traj[128 * p:128 * p + 128] = lines.reshape(128, 1, 128)
    one, two, three = split_bf16(gath[:, SHOTS:, :].reshape(256, 128))
    flat6 = jnp.concatenate([one, one, two, two, one, three], 1)
    shot_row = lax.broadcasted_iota(jnp.int32, (128, 128), 0) // PB
    columns = pl.ds(pl.multiple_of(half * HALF, HALF), HALF)
    for s in range(SHOTS):
        b1, b2, b3 = [jnp.where(shot_row == s, basx_ref[i, :, columns].astype(F32), 0.0).astype(BF) for i in range(3)]
        mixed = jnp.dot(flat6, jnp.concatenate([b1, b2, b1, b2, b3, b1], 0), preferred_element_type=F32)
        mixes[16 * s:16 * s + 16] = mixed.reshape(16, PB, 128)

    lane = lax.broadcasted_iota(jnp.int32, (1, HALF), 1)
    coil = lax.rem(lane // 4, 4)
    masks = [jnp.where(coil == c, 1.0, 0.0).astype(BF) for c in range(4)]
    first = lane < 64
    kline = lax.broadcasted_iota(jnp.int32, (IMG, HALF), 0).astype(F32)

    def prepare(j, p, weights):
        pick = jnp.where(kline == traj[plan_ref[4, j]], 1.0, 0.0).astype(BF)
        cosine = jnp.dot(line_ref[0], pick, preferred_element_type=F32)
        sine = jnp.dot(line_ref[1], pick, preferred_element_type=F32)
        table = jnp.where(first, cosine, sine).astype(BF)
        for c in range(4):
            weights[:, c * YB:(c + 1) * YB, :] = (table * masks[c]).reshape(4, YB, HALF)

    def combine(j, p, slot, weights):
        one, two, three = split_bf16(mixes[plan_ref[5, j]])
        mixed6 = jnp.concatenate([one, two, one, two, three, one], 0)
        rhs = []
        for s in range(2):
            rows = jnp.concatenate([recv[p, w, s, slot] for w in range(4)], 0)
            swapped = jnp.concatenate([-rows[:, HALF:], rows[:, :HALF]], 1)
            rhs.append(jnp.concatenate([rows, swapped], 0))
        for b in range(IMG // YB):
            turns = jnp.dot(basy_ref[b * YB:(b + 1) * YB, :], mixed6, preferred_element_type=F32)
            sine, cosine = sincos_turns(turns)
            sums = None
            for s in range(2):
                image = jnp.dot(weights[b], rhs[s], preferred_element_type=F32)
                for c in range(4):
                    ire, iim = image[c * YB:(c + 1) * YB, :HALF], image[c * YB:(c + 1) * YB, HALF:]
                    rows = slice(c * YB, (c + 1) * YB)
                    terms = (ire + iim) * sens[s, 0, b, rows], iim * sens[s, 1, b, rows], ire * sens[s, 2, b, rows]
                    sums = terms if sums is None else tuple(u + v for u, v in zip(sums, terms))
            ure, uim = sums[0] - sums[1], sums[0] - sums[2]
            contrib[j, b, :, :HALF] = cosine * ure + sine * uim
            contrib[j, b, :, HALF:] = cosine * uim - sine * ure

    prepare(0, 0, weights_a)

    def work(c, carry):
        for n in range(len(every)):
            chunk_copy(c, n).wait_recv()
        for p in range(2):
            self_copy(c, p).wait()

        def pair(k, carry):
            i = c * part + k
            prepare(2 * i + 1, 1, weights_b)
            combine(2 * i, 0, i, weights_a)
            prepare(2 * i + 2, 0, weights_a)
            combine(2 * i + 1, 1, i, weights_b)
            return carry

        lax.fori_loop(0, part, pair, 0)
        return carry

    lax.fori_loop(0, CHUNKS, work, 0)

    def shots(o, b):
        total = None
        for s in range(6):
            term = contrib[plan_ref[6, o * SHOTS + s], b] * plan_ref[7, o * SHOTS + s].astype(F32)
            total = term if total is None else total + term
        return total

    def group(t):
        return lax.rem(x - zh + t + 4, 4) * 4

    ring = ((1, 0), (3, 2))
    relays, blocks, pieces = [], [], []
    for t in range(4):
        for way, (r, k0) in enumerate(ring):
            for k in range(2):
                relay_out[t, way, k] = shots(group(t) + k0 + k, lax.rem(y + 2, 4)).astype(BF)
            copy = remote(relay_out.at[t, way], relay_in.at[t, way], relay_sems, t * 2 + way, along(r))
            copy.start()
            relays.append(copy)
    for t in range(4):
        for way, (r, k0) in enumerate(ring):
            there = lax.rem(y + r, 4)
            relays[t * 2 + way].wait_recv()
            for k in range(4):
                total = shots(group(t) + k, there)
                if k0 <= k < k0 + 2:
                    total = total + relay_in[t, way, k - k0].astype(F32)
                block_out[t, way, k] = total.astype(BF)
            copy = remote(block_out.at[t, way], block_in.at[t, way], block_sems, t * 2 + way, along(r))
            copy.start()
            blocks.append(copy)
    for t in range(4):
        blocks[t * 2].wait_recv()
        blocks[t * 2 + 1].wait_recv()
        for dz in range(4):
            there = lax.rem(zh + dz, 4)
            total = shots(group(t) + there, y) + block_in[t, 0, there].astype(F32) + block_in[t, 1, there].astype(F32)
            for dc in range(2):
                n = (t * 4 + dz) * 2 + dc
                zs[n * 2:n * 2 + 2] = total.astype(BF).reshape(2, 32, IMG)
                to = 1 - core if dc else core
                if n:
                    copy = remote(zs.at[n * 2 + to], zr.at[n], (zsend, zrecv), n, far(dz, (dz + t) % 4, dc))
                    copy.start()
                    pieces.append(copy)
                else:
                    zr[0] = zs[to]
    for copy in pieces:
        copy.wait_recv()
    for dc in range(2):
        e = 1 - core if dc else core
        for odd in range(2):
            column = lax.rem(x + odd, 2)
            total = None
            for n, (dz, dx, c) in enumerate(shifts):
                if c == dc and dx % 2 == odd:
                    total = zr[n].astype(F32) if total is None else total + zr[n].astype(F32)
            out_ref[e, :, pl.ds(pl.multiple_of(column * HALF, HALF), HALF)] = total[:, :HALF]
            out_ref[e, :, pl.ds(pl.multiple_of(IMG + column * HALF, HALF), HALF)] = total[:, HALF:]
    for copy in relays + blocks + pieces:
        copy.wait_send()

    def sent(c, carry):
        for n in range(len(every)):
            chunk_copy(c, n).wait_send()
        return carry

    lax.fori_loop(0, CHUNKS, sent, 0)


def combined(slots, ident, plan, traj, coefs, tab, line, basy, basx, kspace, sens):
    any_ = pl.BlockSpec(memory_space=pl.ANY)
    vm = pl.BlockSpec(memory_space=pltpu.VMEM)
    sm = pl.BlockSpec(memory_space=pltpu.SMEM)
    dma = pltpu.SemaphoreType.DMA
    return pl.pallas_call(
        functools.partial(kernel, slots),
        in_specs=[sm] + [vm] * 6 + [any_, any_],
        out_specs=vm,
        out_shape=jax.ShapeDtypeStruct((2, 32, 2 * IMG), F32),
        scratch_shapes=[
            pltpu.VMEM((24, 128), F32),
            pltpu.VMEM((DIRS * SHOTS, 4, 4, 2 * IMG), BF),
            pltpu.VMEM((8, 2, slots, 16, IMG), BF),
            pltpu.VMEM((2, 4, 2, slots, 16, IMG), BF),
            pltpu.VMEM((2, 4, IMG, IMG), BF),
            pltpu.VMEM((16, 24, 128), F32),
            pltpu.VMEM((2 * slots, 4, YB, IMG), F32),
            pltpu.VMEM((2, 3, 4, 4 * YB, HALF), F32),
            pltpu.VMEM((4, 4 * YB, HALF), BF),
            pltpu.VMEM((4, 4 * YB, HALF), BF),
            pltpu.VMEM((256, 1, 128), F32),
            pltpu.VMEM((128, PB, 128), F32),
            pltpu.VMEM((4, 2, 2, YB, IMG), BF),
            pltpu.VMEM((4, 2, 2, YB, IMG), BF),
            pltpu.VMEM((4, 2, 4, YB, IMG), BF),
            pltpu.VMEM((4, 2, 4, YB, IMG), BF),
            pltpu.VMEM((64, 32, IMG), BF),
            pltpu.VMEM((32, 32, IMG), BF),
            dma((8,)),
            dma((2,)),
            dma((2, CHUNKS)),
            dma((14, CHUNKS)),
            dma((14, CHUNKS)),
            dma((17,)),
            dma((17,)),
            [dma((8,)), dma((8,))],
            [dma((8,)), dma((8,))],
            dma((32,)),
            dma((32,)),
        ],
        compiler_params=pltpu.CompilerParams(collective_id=ident, has_side_effects=True, vmem_limit_bytes=67000000),
        cost_estimate=pl.CostEstimate(flops=2 * slots * 4096 * 256 * 256, bytes_accessed=16 << 20, transcendentals=0),
        name="combined",
    )(plan, traj, coefs, tab, line, basy, basx, kspace, sens)


def plan_kernel(accept_ref, plan_ref):
    mine = lax.axis_index("zl") * 2 + lax.axis_index("core")

    def iota(shape, axis):
        return lax.broadcasted_iota(jnp.int32, shape, axis)

    def flag(cond):
        return jnp.where(cond, 1.0, 0.0)

    tile = flag(lax.rem(iota((SHOTS, 128), 1), SHOTS) == iota((SHOTS, 128), 0)).astype(BF)
    flags = jnp.dot(accept_ref[...].astype(F32).astype(BF), tile, preferred_element_type=F32)
    lane = iota((1, 128), 1)
    o, s = lane // SHOTS, lax.rem(lane, SHOTS)
    first = lax.rem(o, 4) * 16 + lax.rem(o // 4 + o, 4) * 2
    row = iota((8, 128), 0)
    kept = jnp.zeros((8, 128), F32)
    for q in range(4):
        listed = iota((DIRS, 128), 0) == first + (q // 2) * 8 + q % 2
        kept = kept + jnp.where(row == q, jnp.sum(jnp.where(listed, flags, 0.0), 0, keepdims=True), 0.0)
    a, b = iota((128, 128), 0), iota((128, 128), 1)
    keptb = kept.astype(BF)
    upto = jnp.dot(keptb, flag(a <= b).astype(BF), preferred_element_type=F32)
    total = jnp.dot(keptb, jnp.ones((128, 128), BF), preferred_element_type=F32)
    count = jnp.dot(keptb, flag(a // SHOTS == b // SHOTS).astype(BF), preferred_element_type=F32)
    begin = jnp.dot((upto - kept).astype(BF), flag(a == b // SHOTS * SHOTS).astype(BF), preferred_element_type=F32)
    place = jnp.where(kept > 0.5, upto - 1.0, -1.0)
    lanef = iota((128, 128), 0).astype(F32)

    def packed(values, where):
        return lax.dot_general(
            values, flag(lanef == where), (((1,), (1,)), ((), ())), preferred_element_type=F32, precision=lax.Precision.HIGHEST
        )

    plan = jnp.zeros((8, 128), F32)
    for q in range(4):
        source = ((first + (q // 2) * 8 + q % 2) * SHOTS + s).astype(F32)
        plan = plan + packed(jnp.where(row == q, source, 0.0), place[q:q + 1])

    def own(v):
        return jnp.sum(jnp.where(row == mine, v, 0.0), 0, keepdims=True)

    codes = jnp.where(row == 4, lane, jnp.where(row == 5, s * 16 + o, 0)).astype(F32)
    plan = plan + packed(codes, own(place))
    plan = plan + jnp.where(row == 4, lax.rem(lane, 2) * 128, 0).astype(F32)
    sf = s.astype(F32)
    take = jnp.minimum(own(begin) + sf, own(total) - 1.0)
    plan = plan + jnp.where(row == 6, take, 0.0) + jnp.where(row == 7, flag(sf < own(count)), 0.0)
    plan_ref[0:8] = plan.astype(jnp.int32)
    plan_ref[8:16] = jnp.broadcast_to(jnp.max(total, 0, keepdims=True), (8, 128)).astype(jnp.int32)


def on_device(kspace, accept, trajectory, phase_coef, sens):
    vm = pl.BlockSpec(memory_space=pltpu.VMEM)
    plan = pl.pallas_call(
        plan_kernel, in_specs=[vm], out_specs=vm, out_shape=jax.ShapeDtypeStruct((16, 128), jnp.int32), name="plan"
    )(accept)

    basis = basis_const()
    b1, b2, b3 = split3(basis / (2.0 * math.pi))
    basy = jnp.asarray(np.concatenate([b1, b1, b2, b2, b1, b3], 1))
    basx = jnp.asarray(np.stack([np.tile(np.asarray(part).T, (SHOTS, 1)) for part in split3(basis)]))
    tab = readout_const()
    line = jnp.stack(jnp.split(line_const(), 2, 1))
    flat = kspace.reshape(DIRS * SHOTS, 4, 4, 2 * IMG)

    def run(ident, slots):
        def branch(flat, plan, trajectory, phase_coef, sens):
            return combined(slots, ident, plan, trajectory, phase_coef, tab, line, basy, basx, flat, sens)

        return branch

    need = plan[8, 0]
    level = sum((need > 2 * s).astype(jnp.int32) for s in LEVELS[:-1])
    return lax.switch(level, [run(i, s) for i, s in enumerate(LEVELS)], flat, plan, trajectory, phase_coef, sens)


def solution(mesh):
    inner = Mesh(mesh.devices.reshape(4, 2, 4, 4, 2), AXES)
    return jax.shard_map(
        on_device,
        mesh=inner,
        in_specs=(
            P(None, None, ("y", "core"), ("zh", "zl", "x"), None),
            P(),
            P(("zh", "zl", "x"), None, None),
            P(("zh", "zl", "x"), None, None, None),
            P(("y", "core"), None, None),
        ),
        out_specs=P(("zh", "zl", "x"), ("y", "core"), None),
        check_vma=False,
    )
```
